32 devices in a mesh: dp: 1 (over z), tp: 32 (over y, x, core).
Axes of the slice: x: 4, y: 4, z: 1, core: 2. Of those that a mesh axis runs over, the one named last changes fastest.
The devices are a block of a 4x4x8 slice.
Arguments:
- x_norm: bfloat16 [2048, 4096], P(('dp', 'tp'))
- grad_y: bfloat16 [2048, 4096], P(('dp', 'tp'))
- u_gate: bfloat16 [2048, 11008], P('dp', 'tp')
- u_up: bfloat16 [2048, 11008], P('dp', 'tp')
- w_gate: bfloat16 [4096, 11008], P(None, 'tp')
- w_up: bfloat16 [4096, 11008], P(None, 'tp')
- w_down: bfloat16 [11008, 4096], P('tp')
- x_in: bfloat16 [2048, 4096], P(('dp', 'tp'))
- gamma: bfloat16 [4096], replicated
- grad_res: bfloat16 [2048, 4096], P(('dp', 'tp'))
- attn_out: bfloat16 [2048, 4096], P('dp', 'tp')
- w_out: bfloat16 [4096, 4096], P('tp')
Outputs:
- output 1: bfloat16 [2048, 4096], P(('dp', 'tp'))
- output 2: bfloat16 [2048, 4096], P('dp', 'tp')
- output 3: float32 [4096, 11008], P('dp', 'tp')
- output 4: float32 [4096, 11008], P('dp', 'tp')
- output 5: float32 [11008, 4096], P(('dp', 'tp'))
- output 6: float32 [4096, 4096], P(('dp', 'tp'))
All inputs are finite; a program needn't handle non-finite values.
Results may differ from the reference program's by a relative error of at most 0.0158273.
Values are sent between devices in bfloat16 or wider.
A program may use at most 768 MiB of HBM per device.

```python
import jax
import jax.numpy as jnp
from jax import lax

HIDDEN = 4096
FFN_DIM = 11008
TOKENS = 2048
NORM_EPS = 1e-5


def setup_inputs(seed: int = 0, part: int = 0) -> dict:
    part_keys = jax.random.split(jax.random.fold_in(jax.random.key(seed), part), 7)
    weight_keys = jax.random.split(jax.random.key(seed + 1), 5)
    xin_keys = jax.random.split(part_keys[4], 2)
    act_shape = (TOKENS, HIDDEN)
    ffn_shape = (TOKENS, FFN_DIM)
    x_norm = jax.random.normal(part_keys[0], act_shape, jnp.float32)
    grad_y = jax.random.normal(part_keys[1], act_shape, jnp.float32)
    u_gate = jax.random.normal(part_keys[2], ffn_shape, jnp.float32)
    u_up = jax.random.normal(part_keys[3], ffn_shape, jnp.float32)
    xin_scale = jnp.exp(jax.random.uniform(xin_keys[0], (TOKENS, 1), jnp.float32, -1.0, 1.0))
    x_in = jax.random.normal(xin_keys[1], act_shape, jnp.float32) * xin_scale
    grad_res = 0.5 * jax.random.normal(part_keys[5], act_shape, jnp.float32)
    attn_out = jax.random.normal(part_keys[6], act_shape, jnp.float32)
    w_gate = jax.random.normal(weight_keys[0], (HIDDEN, FFN_DIM), jnp.float32) * HIDDEN ** -0.5
    w_up = jax.random.normal(weight_keys[1], (HIDDEN, FFN_DIM), jnp.float32) * HIDDEN ** -0.5
    w_down = jax.random.normal(weight_keys[2], (FFN_DIM, HIDDEN), jnp.float32) * FFN_DIM ** -0.5
    w_out = jax.random.normal(weight_keys[3], (HIDDEN, HIDDEN), jnp.float32) * HIDDEN ** -0.5
    gamma = 1.0 + 0.3 * jax.random.normal(weight_keys[4], (HIDDEN,), jnp.float32)
    return dict(
        x_norm=x_norm.astype(jnp.bfloat16),
        grad_y=grad_y.astype(jnp.bfloat16),
        u_gate=u_gate.astype(jnp.bfloat16),
        u_up=u_up.astype(jnp.bfloat16),
        w_gate=w_gate.astype(jnp.bfloat16),
        w_up=w_up.astype(jnp.bfloat16),
        w_down=w_down.astype(jnp.bfloat16),
        x_in=x_in.astype(jnp.bfloat16),
        gamma=gamma.astype(jnp.bfloat16),
        grad_res=grad_res.astype(jnp.bfloat16),
        attn_out=attn_out.astype(jnp.bfloat16),
        w_out=w_out.astype(jnp.bfloat16),
    )


def reference(x_norm, grad_y, u_gate, u_up, w_gate, w_up, w_down, x_in, gamma, grad_res, attn_out, w_out):
    gate_f = u_gate.astype(jnp.float32)
    up_f = u_up.astype(jnp.float32)
    sig_gate = jax.nn.sigmoid(gate_f)
    act_gate = gate_f * sig_gate
    silu_grad = sig_gate * (1.0 + gate_f * (1.0 - sig_gate))
    hidden_z = (act_gate * up_f).astype(jnp.bfloat16)
    gw_down = jnp.dot(hidden_z.T, grad_y, preferred_element_type=jnp.float32)
    grad_h = jnp.dot(grad_y, w_down.T, preferred_element_type=jnp.float32)
    grad_up = (grad_h * act_gate).astype(jnp.bfloat16)
    grad_gate = (grad_h * up_f * silu_grad).astype(jnp.bfloat16)
    grad_x = (jnp.dot(grad_gate, w_gate.T, preferred_element_type=jnp.float32)
              + jnp.dot(grad_up, w_up.T, preferred_element_type=jnp.float32)).astype(jnp.bfloat16)
    gw_gate = jnp.dot(x_norm.T, grad_gate, preferred_element_type=jnp.float32)
    gw_up = jnp.dot(x_norm.T, grad_up, preferred_element_type=jnp.float32)
    xin_f = x_in.astype(jnp.float32)
    inv_rms = lax.rsqrt(jnp.mean(xin_f * xin_f, axis=-1, keepdims=True) + NORM_EPS)
    scaled = grad_x.astype(jnp.float32) * gamma.astype(jnp.float32)
    proj_mean = jnp.mean(scaled * xin_f, axis=-1, keepdims=True)
    grad_sum = (grad_res.astype(jnp.float32)
                + inv_rms * (scaled - xin_f * (inv_rms * inv_rms) * proj_mean)).astype(jnp.bfloat16)
    grad_attn = jnp.dot(grad_sum, w_out.T, preferred_element_type=jnp.float32).astype(jnp.bfloat16)
    gw_out = jnp.dot(attn_out.T, grad_sum, preferred_element_type=jnp.float32)
    return grad_sum, grad_attn, gw_gate, gw_up, gw_down, gw_out
```

```python
import functools
import math

import jax
import jax.numpy as jnp
from jax import lax
from jax.experimental import pallas as pl
from jax.experimental.pallas import tpu as pltpu
from jax.sharding import PartitionSpec as P

NORM_EPS = 1e-5
F32, BF16 = jnp.float32, jnp.bfloat16
LAG_X = 3
LAG_R = 2
SUBS = 4
SLOTS = 6
NN = (((1,), (0,)), ((), ()))
NT = (((1,), (1,)), ((), ()))
TN = (((0,), (0,)), ((), ()))


def dot(a, b, dims):
    return lax.dot_general(a, b, dims, preferred_element_type=F32)


def kernel(side, x_in_hbm, gy_in_hbm, ug_hbm, uu_hbm, wg_hbm, wu_hbm, wd_hbm, xin_hbm, gamma_hbm, gr_hbm, o_hbm, wo_hbm,
           ds_out, do_out, dwg_out, dwu_out, dwd_out, dwo_out,
           yb, xb, ugt, uut, ug, uu, wg, wu, wd, xin, gamma, gr, ov, wo,
           acc_g, acc_u, acc_d, acc_o, g_s, du_g, du_u, z_s, own_part, pp_send, pp_recv, rs_send, rs_recv, acc0,
           do_v, do_acc, o_pair,
           y_rs, y_rr, y_ps, y_pr, x_rs, x_rr, x_ps, x_pr,
           s_rs, s_rr, s_ps, s_pr, r_s, r_r, q_s, q_r, loc):
    n = side * side
    tok, hid = x_in_hbm.shape
    half = tok // 2
    ct = hid // 8
    sub_w = hid // SUBS

    me = lax.axis_index("tp")
    core = me % 2
    chip = me // 2
    cy, cx = chip // side, chip % side
    diag = (cx + cy) % side
    pos_own = side * (cy * (1 - core) + cx * core) + diag
    pos_par = side * (cx * (1 - core) + cy * core) + diag

    def index_of(e, q):
        a, b = q // side, q % side
        o = (b - a + side) % side
        yy = a * (1 - e) + o * e
        xx = o * (1 - e) + a * e
        return (yy * side + xx) * 2 + e

    partner = me + 1 - 2 * core
    nxt = (index_of(core, (pos_own + 1) % n), index_of(core, (pos_own + n - 1) % n))

    def token_row(s, rel, d):
        e = core if rel == 0 else 1 - core
        base = pos_own if rel == 0 else pos_par
        q = (base + n - s) % n if d == 0 else (base + s) % n
        return pl.multiple_of(index_of(e, q) * tok + half * d, half)

    def remote(src, dst, ssem, rsem, dev):
        return pltpu.make_async_remote_copy(src_ref=src, dst_ref=dst, send_sem=ssem, recv_sem=rsem,
                                            device_id={"tp": dev}, device_id_type=pl.DeviceIdType.MESH)

    def local(i):
        pairs = ((gy_in_hbm, yb.at[0, pl.ds(0, tok), :]), (x_in_hbm, xb.at[0, pl.ds(0, tok), :]),
                 (wd_hbm, wd), (ug_hbm, ugt), (uu_hbm, uut), (wg_hbm, wg), (wu_hbm, wu),
                 (xin_hbm, xin), (gamma_hbm, gamma), (gr_hbm, gr), (o_hbm, ov), (wo_hbm, wo),
                 (acc_d, dwd_out), (acc_g, dwg_out), (acc_u, dwu_out),
                 (yb.at[0, pl.ds(0, tok), :], ds_out), (do_v, do_out), (acc_o, dwo_out))
        return pltpu.make_async_copy(pairs[i][0], pairs[i][1], loc.at[i])

    for i in range(12):
        local(i).start()

    barrier = pltpu.get_barrier_semaphore()
    for dev in (nxt[0], nxt[1], partner):
        pl.semaphore_signal(barrier, inc=1, device_id={"tp": dev}, device_id_type=pl.DeviceIdType.MESH)
    pl.semaphore_wait(barrier, 3)

    def rows_at(s, rel, d):
        return pl.ds(pl.multiple_of((s % 2) * (2 * tok) + rel * tok + d * half, half), half)

    def ring_copy(b, ss, rr, s, d, cols=None):
        c = pl.ds(0, hid) if cols is None else cols
        return remote(b.at[(s // 2) % 3, rows_at(s, 0, d), c], b.at[((s + 1) // 2) % 3, rows_at(s + 1, 0, d), c],
                      ss(s, d), rr(s + 1, d), nxt[d])

    def pair_copy(b, ss, rr, s, d, cols=None):
        c = pl.ds(0, hid) if cols is None else cols
        return remote(b.at[(s // 2) % 3, rows_at(s, 0, d), c], b.at[(s // 2) % 3, rows_at(s, 1, d), c],
                      ss(s, d), rr(s, d), partner)

    def sem_of(arr):
        return lambda s, d: arr.at[d, s % SLOTS]

    def gather_service(b, sems, s, first):
        rs, rr, ps, pr = (sem_of(a) for a in sems)

        @pl.when(jnp.logical_and(s >= 2, s <= n + 1))
        def _():
            for d in range(2):
                pair_copy(b, ps, pr, s - 2, d).wait_send()

        @pl.when(jnp.logical_and(s >= 2, s <= n))
        def _():
            for d in range(2):
                ring_copy(b, rs, rr, s - 2, d).wait_send()

        @pl.when(s == 0)
        def _():
            local(first).wait()

        for d in range(2):
            @pl.when(jnp.logical_and(s >= 1, s <= n - 1))
            def _():
                ring_copy(b, rs, rr, s - 1, d).wait_recv()

            @pl.when(jnp.logical_and(s >= 0, s <= n - 2))
            def _():
                ring_copy(b, rs, rr, s, d).start()

            @pl.when(jnp.logical_and(s >= 0, s <= n - 1))
            def _():
                pair_copy(b, ps, pr, s, d).start()

        @pl.when(jnp.logical_and(s >= 0, s <= n - 1))
        def _():
            for d in range(2):
                pair_copy(b, ps, pr, s, d).wait_recv()

    y_sems, x_sems = (y_rs, y_rr, y_ps, y_pr), (x_rs, x_rr, x_ps, x_pr)

    def part_a(t):
        gather_service(yb, y_sems, t, 0)

    def part_b(t):
        gather_service(xb, x_sems, t - LAG_X, 1)

    def task_1(k):
        @pl.when(k == 0)
        def _():
            for i in (2, 3, 4):
                local(i).wait()

            def turn(c, carry):
                cols = pl.ds(pl.multiple_of(c * 128, 128), 128)
                ug[cols, :] = ugt[:, cols].astype(F32).T.astype(BF16)
                uu[cols, :] = uut[:, cols].astype(F32).T.astype(BF16)
                return carry
            lax.fori_loop(0, ug.shape[0] // 128, turn, 0)
        g_s[...] = dot(yb[k % 3], wd[...], NT)
        for i in range(2):
            for rel in range(2):
                for d in range(2):
                    r0 = i * 2 * tok + rel * tok + d * half
                    row = token_row(2 * k + i, rel, d)
                    gate = ug[pl.ds(row, half), :].astype(F32)
                    up = uu[pl.ds(row, half), :].astype(F32)
                    sig = jax.nn.sigmoid(gate)
                    act = gate * sig
                    grad = g_s[pl.ds(r0, half), :]
                    z_s[pl.ds(r0, half), :] = (act * up).astype(BF16)
                    du_u[k % 2, pl.ds(r0, half), :] = (grad * act).astype(BF16)
                    du_g[k % 2, pl.ds(r0, half), :] = (grad * up * (sig * (1.0 + gate * (1.0 - sig)))).astype(BF16)

    def pp_copy(k):
        return remote(pp_send.at[k % 2], pp_recv.at[k % 2], q_s.at[k % 2], q_r.at[k % 2], partner)

    def task_2(k, lo, hi):
        ks = k % 2
        if lo == 0:
            @pl.when(k == 0)
            def _():
                local(5).wait()
                local(6).wait()

            @pl.when(k >= 2)
            def _():
                pp_copy(k - 2).wait_send()

        def body(c, carry):
            cols = pl.ds(pl.multiple_of(c * ct, ct), ct)
            r = (dot(du_g[ks], wg[:, cols], NN) + dot(du_u[ks], wu[:, cols], NN)).astype(BF16)
            for i in range(2):
                own_part[ks, pl.ds(i * tok, tok), cols] = r[i * 2 * tok:i * 2 * tok + tok]
                pp_send[ks, pl.ds(i * tok, tok), cols] = r[i * 2 * tok + tok:(i + 1) * 2 * tok]
            return carry
        lax.fori_loop(lo, hi, body, 0)
        if hi == 8:
            pp_copy(k).start()

    def task_3(k):
        def body(c, carry):
            cols = pl.ds(pl.multiple_of(c * ct, ct), ct)
            acc_d[:, cols] += dot(z_s[...], yb[k % 3, :, cols], TN)
            return carry
        lax.fori_loop(0, 8, body, 0)

    def task_4(k):
        def body(c, carry):
            cols = pl.ds(pl.multiple_of(c * ct, ct), ct)
            xt = xb[k % 3, :, cols]
            acc_g[:, cols] += dot(du_g[k % 2], xt, TN)
            acc_u[:, cols] += dot(du_u[k % 2], xt, TN)
            return carry
        lax.fori_loop(0, 8, body, 0)

    def rs_copy(j, d):
        return remote(rs_send.at[j % 2, pl.ds(d * half, half), :], rs_recv.at[(j + 1) % 3, pl.ds(d * half, half), :],
                      r_s.at[d, j % 2], r_r.at[d, (j + 1) % 3], nxt[d])

    def part_d(t, i):
        j = t - LAG_R
        ks = (j // 2) % 2
        rows = pl.ds(i * tok, tok)
        if i == 0:
            @pl.when(jnp.logical_and(j >= 0, j <= n - 2))
            def _():
                pp_copy(j // 2).wait_recv()

            @pl.when(j == 0)
            def _():
                acc0[...] = own_part[ks, rows, :].astype(F32) + pp_recv[ks, rows, :].astype(F32)

        @pl.when(jnp.logical_and(j >= 3, j <= n + 1))
        def _():
            for d in range(2):
                rs_copy(j - 2, d).wait_send()

        for d in range(2):
            dr = pl.ds(d * half, half)
            pr = pl.ds(i * tok + d * half, half)

            @pl.when(jnp.logical_and(j >= 2, j <= n))
            def _():
                rs_copy(j - 1, d).wait_recv()

            @pl.when(j == 1)
            def _():
                rs_send[j % 2, dr, :] = (own_part[ks, pr, :].astype(F32) + pp_recv[ks, pr, :].astype(F32)).astype(BF16)

            @pl.when(jnp.logical_and(j >= 2, j <= n - 1))
            def _():
                rs_send[j % 2, dr, :] = (own_part[ks, pr, :].astype(F32) + pp_recv[ks, pr, :].astype(F32)
                                         + rs_recv[j % 3, dr, :].astype(F32)).astype(BF16)

            @pl.when(jnp.logical_and(j >= 1, j <= n - 1))
            def _():
                rs_copy(j, d).start()

    acc_d[...] = jnp.zeros_like(acc_d)
    acc_g[...] = jnp.zeros_like(acc_g)
    acc_u[...] = jnp.zeros_like(acc_u)
    acc_o[...] = jnp.zeros_like(acc_o)

    def pair_body(kk, carry):
        t = 2 * kk
        part_a(t)

        @pl.when(jnp.logical_and(kk >= 1, kk <= 8))
        def _():
            task_3(kk - 1)
        part_d(t, 0)
        part_b(t)

        @pl.when(kk >= 2)
        def _():
            task_4(kk - 2)
        t = 2 * kk + 1
        part_a(t)

        @pl.when(kk <= 7)
        def _():
            task_1(kk)
        part_d(t, 1)

        @pl.when(kk <= 7)
        def _():
            task_2(kk, 0, 4)
        part_b(t)

        @pl.when(kk <= 7)
        def _():
            task_2(kk, 4, 8)
        return carry

    lax.fori_loop(0, n // 2 + 2, pair_body, 0)
    for d in range(2):
        pair_copy(xb, sem_of(x_ps), sem_of(x_pr), n - 1, d).wait_send()
    pp_copy(n // 2 - 2).wait_send()
    pp_copy(n // 2 - 1).wait_send()
    for i in range(12, 15):
        local(i).start()

    for i in (7, 8, 9, 10, 11):
        local(i).wait()

    def norm(c, carry):
        rows = pl.ds(pl.multiple_of(c * 16, 16), 16)
        xf = xin[rows, :].astype(F32)
        inv = lax.rsqrt(jnp.mean(xf * xf, axis=-1, keepdims=True) + NORM_EPS)
        gx = (acc0[rows, :] + rs_recv[n % 3, rows, :].astype(F32)).astype(BF16)
        scaled = gx.astype(F32) * gamma[...].astype(F32)
        proj = jnp.mean(scaled * xf, axis=-1, keepdims=True)
        yb[0, rows, :] = (gr[rows, :].astype(F32) + inv * (scaled - xf * (inv * inv) * proj)).astype(BF16)
        return carry
    lax.fori_loop(0, tok // 16, norm, 0)
    local(15).start()

    def s_sem(arr, c):
        return lambda s, d: arr.at[d, c, s % 4]

    def o_task(m, c):
        cols = pl.ds(pl.multiple_of(c * ct, ct), ct)
        blk = yb[m % 3, :, cols]
        acc_o[:, cols] += dot(o_pair[...], blk, TN)
        part = dot(blk, wo[:, cols], NT)

        @pl.when(c == 0)
        def _():
            do_acc[...] = part

        @pl.when(c > 0)
        def _():
            do_acc[...] += part

    def o_rows(m):
        for i in range(2):
            for rel in range(2):
                for d in range(2):
                    yield i * 2 * tok + rel * tok + d * half, token_row(2 * m + i, rel, d)

    def o_begin(m):
        for r0, row in o_rows(m):
            o_pair[pl.ds(r0, half), :] = ov[pl.ds(row, half), :]

    def o_end(m):
        for r0, row in o_rows(m):
            do_v[pl.ds(row, half), :] = do_acc[pl.ds(r0, half), :].astype(BF16)

    def s_step(u, carry):
        m = u // 2 - 1

        @pl.when(u == 2)
        def _():
            local(15).wait()

        @pl.when(jnp.logical_and(u >= 2, u % 2 == 0))
        def _():
            o_begin(m)
        for c in range(SUBS):
            cols = pl.ds(c * sub_w, sub_w)
            rs, rr, ps, pr = (s_sem(a, c) for a in (s_rs, s_rr, s_ps, s_pr))
            for d in range(2):
                @pl.when(jnp.logical_and(u >= 2, u <= n + 1))
                def _():
                    pair_copy(yb, ps, pr, u - 2, d, cols).wait_send()

                @pl.when(jnp.logical_and(u >= 2, u <= n))
                def _():
                    ring_copy(yb, rs, rr, u - 2, d, cols).wait_send()

                @pl.when(jnp.logical_and(u >= 1, u <= n - 1))
                def _():
                    ring_copy(yb, rs, rr, u - 1, d, cols).wait_recv()

                @pl.when(u <= n - 2)
                def _():
                    ring_copy(yb, rs, rr, u, d, cols).start()

                @pl.when(u <= n - 1)
                def _():
                    pair_copy(yb, ps, pr, u, d, cols).start()

            @pl.when(u >= 2)
            def _():
                o_task(m, (u % 2) * SUBS + c)

        for c in range(SUBS):
            cols = pl.ds(c * sub_w, sub_w)
            for d in range(2):
                @pl.when(u <= n - 1)
                def _():
                    pair_copy(yb, s_sem(s_ps, c), s_sem(s_pr, c), u, d, cols).wait_recv()

        @pl.when(jnp.logical_and(u >= 2, u % 2 == 1))
        def _():
            o_end(m)
        return carry

    lax.fori_loop(0, n + 2, s_step, 0)
    local(16).start()
    local(17).start()
    for i in (12, 13, 14, 16, 17):
        local(i).wait()


def mega(side, *args):
    tok, hid = args[0].shape
    fl, rows = args[2].shape
    ol = args[10].shape[1]
    dma = pltpu.SemaphoreType.DMA
    ring = [dma((2, SLOTS)) for _ in range(8)] + [dma((2, SUBS, 4)) for _ in range(4)]
    sems = ring + [dma((2, 2)), dma((2, 3)), dma((2,)), dma((2,)), dma((18,))]
    out_shape = (
        jax.ShapeDtypeStruct((tok, hid), BF16), jax.ShapeDtypeStruct((rows, ol), BF16),
        jax.ShapeDtypeStruct((fl, hid), F32), jax.ShapeDtypeStruct((fl, hid), F32),
        jax.ShapeDtypeStruct((fl, hid), F32), jax.ShapeDtypeStruct((ol, hid), F32))
    v = pltpu.VMEM
    blk = 4 * tok
    scratch = [
        v((3, blk, hid), BF16), v((3, blk, hid), BF16), v((fl, rows), BF16), v((fl, rows), BF16), v((rows, fl), BF16), v((rows, fl), BF16),
        v((fl, hid), BF16), v((fl, hid), BF16), v((fl, hid), BF16), v((tok, hid), BF16), v((1, hid), BF16),
        v((tok, hid), BF16), v((rows, ol), BF16), v((ol, hid), BF16),
        v((fl, hid), F32), v((fl, hid), F32), v((fl, hid), F32), v((ol, hid), F32),
        v((blk, fl), F32), v((2, blk, fl), BF16), v((2, blk, fl), BF16), v((blk, fl), BF16),
        v((2, 2 * tok, hid), BF16), v((2, 2 * tok, hid), BF16), v((2, 2 * tok, hid), BF16),
        v((2, tok, hid), BF16), v((3, tok, hid), BF16), v((tok, hid), F32),
        v((rows, ol), BF16), v((blk, ol), F32), v((blk, ol), BF16)]
    anyspec = pl.BlockSpec(memory_space=pl.ANY)
    return pl.pallas_call(
        functools.partial(kernel, side),
        out_shape=out_shape,
        in_specs=[anyspec] * 12,
        out_specs=tuple([anyspec] * 6),
        scratch_shapes=scratch + sems,
        compiler_params=pltpu.CompilerParams(collective_id=0, has_side_effects=True, vmem_limit_bytes=67043328),
    )(*args)


def solution(mesh):
    token_spec = P(("dp", "tp"), None)
    split_cols = P("dp", "tp")
    weight_cols = P(None, "tp")
    weight_rows = P("tp", None)
    side = math.isqrt(mesh.shape["tp"] // 2)

    def local_backward(x_norm, grad_y, u_gate, u_up, w_gate, w_up, w_down, x_in, gamma, grad_res, attn_out, w_out):
        grad_sum, grad_attn, gw_gate, gw_up, gw_down, gw_out = mega(
            side, x_norm, grad_y, u_gate.T, u_up.T, w_gate.T, w_up.T, w_down, x_in, gamma.reshape(1, -1),
            grad_res, attn_out, w_out)
        return grad_sum, grad_attn, gw_gate.T, gw_up.T, gw_down, gw_out

    return jax.shard_map(
        local_backward,
        mesh=mesh,
        in_specs=(token_spec, token_spec, split_cols, split_cols, weight_cols, weight_cols, weight_rows,
                  token_spec, P(None), token_spec, split_cols, weight_rows),
        out_specs=(token_spec, split_cols, split_cols, split_cols, token_spec, token_spec),
        check_vma=False,
    )
```

```python
import functools
import math

import jax
import jax.numpy as jnp
from jax import lax
from jax.experimental import pallas as pl
from jax.experimental.pallas import tpu as pltpu
from jax.sharding import PartitionSpec as P

NORM_EPS = 1e-5
F32, BF16 = jnp.float32, jnp.bfloat16
LAG_X = 2
LAG_R = 2
PIECES = 2
SUBS = 4
SLOTS = 6
NN = (((1,), (0,)), ((), ()))
NT = (((1,), (1,)), ((), ()))
TN = (((0,), (0,)), ((), ()))


def dot(a, b, dims):
    return lax.dot_general(a, b, dims, preferred_element_type=F32)


def kernel(side, x_in_hbm, gy_in_hbm, ug_hbm, uu_hbm, wg_hbm, wu_hbm, wd_hbm, xin_hbm, gamma_hbm, gr_hbm, o_hbm, wo_hbm,
           ds_out, do_v, acc_g, acc_u, acc_d, acc_o,
           yb, xb, ugt, uut, ug, uu, wg, wu, wd, xin, gamma, gr, ov, wo,
           g_s, du_g, du_u, z_s, own_part, pp_send, pp_recv, rs_send, rs_recv, acc0,
           do_acc, o_pair,
           y_rs, y_rr, y_ps, y_pr, x_rs, x_rr, x_ps, x_pr,
           s_rs, s_rr, s_ps, s_pr, r_s, r_r, q_s, q_r, loc):
    n = side * side
    tok, hid = x_in_hbm.shape
    half = tok // 2
    ct = hid // 8

    me = lax.axis_index("tp")
    core = me % 2
    chip = me // 2
    cy, cx = chip // side, chip % side
    diag = (cx + cy) % side
    pos_own = side * (cy * (1 - core) + cx * core) + diag
    pos_par = side * (cx * (1 - core) + cy * core) + diag

    def index_of(e, q):
        a, b = q // side, q % side
        o = (b - a + side) % side
        yy = a * (1 - e) + o * e
        xx = o * (1 - e) + a * e
        return (yy * side + xx) * 2 + e

    partner = me + 1 - 2 * core
    nxt = (index_of(core, (pos_own + 1) % n), index_of(core, (pos_own + n - 1) % n))

    def token_row(s, rel, d):
        e = core if rel == 0 else 1 - core
        base = pos_own if rel == 0 else pos_par
        q = (base + n - s) % n if d == 0 else (base + s) % n
        return pl.multiple_of(index_of(e, q) * tok + half * d, half)

    def remote(src, dst, ssem, rsem, dev):
        return pltpu.make_async_remote_copy(src_ref=src, dst_ref=dst, send_sem=ssem, recv_sem=rsem,
                                            device_id={"tp": dev}, device_id_type=pl.DeviceIdType.MESH)

    def local(i):
        pairs = ((gy_in_hbm, yb.at[0, pl.ds(0, tok), :]), (x_in_hbm, xb.at[0, pl.ds(0, tok), :]),
                 (wd_hbm, wd), (ug_hbm, ugt), (uu_hbm, uut), (wg_hbm, wg), (wu_hbm, wu),
                 (xin_hbm, xin), (gamma_hbm, gamma), (gr_hbm, gr), (o_hbm, ov), (wo_hbm, wo))
        return pltpu.make_async_copy(pairs[i][0], pairs[i][1], loc.at[i])

    for i in range(12):
        local(i).start()

    barrier = pltpu.get_barrier_semaphore()
    for dev in (nxt[0], nxt[1], partner):
        pl.semaphore_signal(barrier, inc=1, device_id={"tp": dev}, device_id_type=pl.DeviceIdType.MESH)
    pl.semaphore_wait(barrier, 3)

    def rows_at(s, rel, d):
        return pl.ds(pl.multiple_of((s % 2) * (2 * tok) + rel * tok + d * half, half), half)

    def cols_of(c, pieces):
        return pl.ds(c * (hid // pieces), hid // pieces)

    def ring_copy(b, sems, s, d, c, pieces):
        cols = cols_of(c, pieces)
        m = sems[0].shape[2]
        return remote(b.at[(s // 2) % 3, rows_at(s, 0, d), cols], b.at[((s + 1) // 2) % 3, rows_at(s + 1, 0, d), cols],
                      sems[0].at[d, c, s % m], sems[1].at[d, c, (s + 1) % m], nxt[d])

    def pair_copy(b, sems, s, d, c, pieces):
        cols = cols_of(c, pieces)
        m = sems[0].shape[2]
        return remote(b.at[(s // 2) % 3, rows_at(s, 0, d), cols], b.at[(s // 2) % 3, rows_at(s, 1, d), cols],
                      sems[2].at[d, c, s % m], sems[3].at[d, c, s % m], partner)

    def between(s, lo, hi):
        return jnp.logical_and(s >= lo, s <= hi)

    def each(pieces, f):
        for c in range(pieces):
            for d in range(2):
                f(d, c, pieces)

    def forward(b, sems, s, first):
        @pl.when(s == 0)
        def _():
            local(first).wait()

        def one(d, c, pieces):
            @pl.when(between(s, 1, n - 1))
            def _():
                ring_copy(b, sems, s - 1, d, c, pieces).wait_recv()

            @pl.when(between(s, 0, n - 2))
            def _():
                ring_copy(b, sems, s, d, c, pieces).start()

            @pl.when(between(s, 0, n - 1))
            def _():
                pair_copy(b, sems, s, d, c, pieces).start()
        each(PIECES, one)

        @pl.when(between(s, 2, n + 1))
        def _():
            each(PIECES, lambda d, c, p: pair_copy(b, sems, s - 2, d, c, p).wait_send())

        @pl.when(between(s, 2, n))
        def _():
            each(PIECES, lambda d, c, p: ring_copy(b, sems, s - 2, d, c, p).wait_send())

    def pair_wait(b, sems, s):
        each(PIECES, lambda d, c, p: pair_copy(b, sems, s, d, c, p).wait_recv())

    y_sems, x_sems, s_sems = (y_rs, y_rr, y_ps, y_pr), (x_rs, x_rr, x_ps, x_pr), (s_rs, s_rr, s_ps, s_pr)

    def part_a(t):
        forward(yb, y_sems, t, 0)

    def part_b(t):
        forward(xb, x_sems, t - LAG_X, 1)

    def task_1(k):
        @pl.when(k == 0)
        def _():
            for i in (2, 3, 4):
                local(i).wait()

            def turn(c, carry):
                cols = pl.ds(pl.multiple_of(c * 128, 128), 128)
                ug[cols, :] = ugt[:, cols].astype(F32).T.astype(BF16)
                uu[cols, :] = uut[:, cols].astype(F32).T.astype(BF16)
                return carry
            lax.fori_loop(0, ug.shape[0] // 128, turn, 0)
        pair_wait(yb, y_sems, 2 * k)
        pair_wait(yb, y_sems, 2 * k + 1)
        g_s[...] = dot(wd[...], yb[k % 3], NT).T
        for i in range(2):
            for rel in range(2):
                for d in range(2):
                    r0 = i * 2 * tok + rel * tok + d * half
                    row = token_row(2 * k + i, rel, d)
                    gate = ug[pl.ds(row, half), :].astype(F32)
                    up = uu[pl.ds(row, half), :].astype(F32)
                    sig = jax.nn.sigmoid(gate)
                    act = gate * sig
                    grad = g_s[pl.ds(r0, half), :]
                    z_s[pl.ds(r0, half), :] = (act * up).astype(BF16)
                    du_u[k % 2, pl.ds(r0, half), :] = (grad * act).astype(BF16)
                    du_g[k % 2, pl.ds(r0, half), :] = (grad * up * (sig * (1.0 + gate * (1.0 - sig)))).astype(BF16)

    def pp_copy(k):
        return remote(pp_send.at[k % 2], pp_recv.at[k % 2], q_s.at[k % 2], q_r.at[k % 2], partner)

    def task_2(k, lo, hi):
        ks = k % 2
        if lo == 0:
            @pl.when(k == 0)
            def _():
                local(5).wait()
                local(6).wait()

            @pl.when(k >= 2)
            def _():
                pp_copy(k - 2).wait_send()

        def body(c, carry):
            cols = pl.ds(pl.multiple_of(c * ct, ct), ct)
            r = (dot(du_g[ks], wg[:, cols], NN) + dot(du_u[ks], wu[:, cols], NN)).astype(BF16)
            for i in range(2):
                own_part[ks, pl.ds(i * tok, tok), cols] = r[i * 2 * tok:i * 2 * tok + tok]
                pp_send[ks, pl.ds(i * tok, tok), cols] = r[i * 2 * tok + tok:(i + 1) * 2 * tok]
            return carry
        lax.fori_loop(lo, hi, body, 0)
        if hi == 8:
            pp_copy(k).start()

    def task_3(k):
        def body(c, carry):
            cols = pl.ds(pl.multiple_of(c * ct, ct), ct)
            acc_d[:, cols] += dot(z_s[...], yb[k % 3, :, cols], TN)
            return carry
        lax.fori_loop(0, 8, body, 0)

    def task_4(k, lo, hi):
        if lo == 0:
            pair_wait(xb, x_sems, 2 * k)
            pair_wait(xb, x_sems, 2 * k + 1)

        def body(c, carry):
            cols = pl.ds(pl.multiple_of(c * ct, ct), ct)
            xt = xb[k % 3, :, cols]
            acc_g[:, cols] += dot(du_g[k % 2], xt, TN)
            acc_u[:, cols] += dot(du_u[k % 2], xt, TN)
            return carry
        lax.fori_loop(lo, hi, body, 0)

    def rs_copy(j, d, c, pieces):
        rows, cols = pl.ds(d * half, half), cols_of(c, pieces)
        return remote(rs_send.at[j % 2, rows, cols], rs_recv.at[(j + 1) % 3, rows, cols],
                      r_s.at[d, c, j % 2], r_r.at[d, c, (j + 1) % 3], nxt[d])

    def part_d(t, i):
        j = t - LAG_R
        ks = (j // 2) % 2
        rows = pl.ds(i * tok, tok)
        if i == 0:
            @pl.when(between(j, 0, n - 2))
            def _():
                pp_copy(j // 2).wait_recv()

            @pl.when(j == 0)
            def _():
                acc0[...] = own_part[ks, rows, :].astype(F32) + pp_recv[ks, rows, :].astype(F32)

        @pl.when(between(j, 3, n + 1))
        def _():
            each(PIECES, lambda d, c, p: rs_copy(j - 2, d, c, p).wait_send())

        def one(d, c, pieces):
            dr = pl.ds(d * half, half)
            pr = pl.ds(i * tok + d * half, half)
            cols = cols_of(c, pieces)

            @pl.when(between(j, 2, n))
            def _():
                rs_copy(j - 1, d, c, pieces).wait_recv()

            @pl.when(j == 1)
            def _():
                rs_send[j % 2, dr, cols] = (own_part[ks, pr, cols].astype(F32)
                                            + pp_recv[ks, pr, cols].astype(F32)).astype(BF16)

            @pl.when(between(j, 2, n - 1))
            def _():
                rs_send[j % 2, dr, cols] = (own_part[ks, pr, cols].astype(F32) + pp_recv[ks, pr, cols].astype(F32)
                                            + rs_recv[j % 3, dr, cols].astype(F32)).astype(BF16)

            @pl.when(between(j, 1, n - 1))
            def _():
                rs_copy(j, d, c, pieces).start()
        each(PIECES, one)

    def pair_body(kk, carry):
        t = 2 * kk
        part_a(t)

        @pl.when(kk == 0)
        def _():
            acc_d[...] = jnp.zeros_like(acc_d)
            acc_g[...] = jnp.zeros_like(acc_g)
            acc_u[...] = jnp.zeros_like(acc_u)
            acc_o[...] = jnp.zeros_like(acc_o)

        @pl.when(kk >= 2)
        def _():
            task_4(kk - 2, 0, 4)
        part_d(t, 0)

        @pl.when(kk >= 2)
        def _():
            task_4(kk - 2, 4, 8)
        part_b(t)
        t = 2 * kk + 1
        part_a(t)

        @pl.when(between(kk, 1, n // 2))
        def _():
            task_3(kk - 1)

        @pl.when(kk < n // 2)
        def _():
            task_1(kk)
        part_d(t, 1)

        @pl.when(kk < n // 2)
        def _():
            task_2(kk, 0, 4)
        part_b(t)

        @pl.when(kk < n // 2)
        def _():
            task_2(kk, 4, 8)
        return carry

    lax.fori_loop(0, n // 2 + 2, pair_body, 0)
    pp_copy(n // 2 - 2).wait_send()
    pp_copy(n // 2 - 1).wait_send()

    for i in (7, 8, 9, 10, 11):
        local(i).wait()

    def norm(c, carry):
        rows = pl.ds(pl.multiple_of(c * 16, 16), 16)
        xf = xin[rows, :].astype(F32)
        inv = lax.rsqrt(jnp.mean(xf * xf, axis=-1, keepdims=True) + NORM_EPS)
        gx = (acc0[rows, :] + rs_recv[n % 3, rows, :].astype(F32)).astype(BF16)
        scaled = gx.astype(F32) * gamma[...].astype(F32)
        proj = jnp.mean(scaled * xf, axis=-1, keepdims=True)
        ds = (gr[rows, :].astype(F32) + inv * (scaled - xf * (inv * inv) * proj)).astype(BF16)
        yb[0, rows, :] = ds
        ds_out[rows, :] = ds
        return carry
    lax.fori_loop(0, tok // 16, norm, 0)

    def o_task(m, c):
        cols = pl.ds(pl.multiple_of(c * ct, ct), ct)
        blk = yb[m % 3, :, cols]
        acc_o[:, cols] += dot(o_pair[...], blk, TN)
        part = dot(blk, wo[:, cols], NT)

        @pl.when(c == 0)
        def _():
            do_acc[...] = part

        @pl.when(c > 0)
        def _():
            do_acc[...] += part

    def o_rows(m):
        for i in range(2):
            for rel in range(2):
                for d in range(2):
                    yield i * 2 * tok + rel * tok + d * half, token_row(2 * m + i, rel, d)

    def o_begin(m):
        for r0, row in o_rows(m):
            o_pair[pl.ds(r0, half), :] = ov[pl.ds(row, half), :]

    def o_end(m):
        for r0, row in o_rows(m):
            do_v[pl.ds(row, half), :] = do_acc[pl.ds(r0, half), :].astype(BF16)

    def s_step(u, carry):
        m = u // 2 - 1

        @pl.when(jnp.logical_and(u >= 2, u % 2 == 0))
        def _():
            each(SUBS, lambda d, c, p: pair_copy(yb, s_sems, 2 * m, d, c, p).wait_recv())
            each(SUBS, lambda d, c, p: pair_copy(yb, s_sems, 2 * m + 1, d, c, p).wait_recv())
            o_begin(m)
        for c in range(SUBS):
            for d in range(2):
                @pl.when(between(u, 1, n - 1))
                def _():
                    ring_copy(yb, s_sems, u - 1, d, c, SUBS).wait_recv()

                @pl.when(u <= n - 2)
                def _():
                    ring_copy(yb, s_sems, u, d, c, SUBS).start()

                @pl.when(u <= n - 1)
                def _():
                    pair_copy(yb, s_sems, u, d, c, SUBS).start()

                @pl.when(between(u, 2, n + 1))
                def _():
                    pair_copy(yb, s_sems, u - 2, d, c, SUBS).wait_send()

                @pl.when(between(u, 2, n))
                def _():
                    ring_copy(yb, s_sems, u - 2, d, c, SUBS).wait_send()

            @pl.when(u >= 2)
            def _():
                o_task(m, (u % 2) * SUBS + c)

        @pl.when(jnp.logical_and(u >= 2, u % 2 == 1))
        def _():
            o_end(m)
        return carry

    lax.fori_loop(0, n + 2, s_step, 0)


def mega(side, *args):
    tok, hid = args[0].shape
    fl, rows = args[2].shape
    ol = args[10].shape[1]
    dma = pltpu.SemaphoreType.DMA
    ring = [dma((2, PIECES, SLOTS)) for _ in range(8)] + [dma((2, SUBS, 4)) for _ in range(4)]
    sems = ring + [dma((2, PIECES, 2)), dma((2, PIECES, 3)), dma((2,)), dma((2,)), dma((12,))]
    out_shape = (pltpu.VMEM((tok, hid), BF16), pltpu.VMEM((rows, ol), BF16), pltpu.VMEM((fl, hid), F32),
                 pltpu.VMEM((fl, hid), F32), pltpu.VMEM((fl, hid), F32), pltpu.VMEM((ol, hid), F32))
    v = pltpu.VMEM
    blk = 4 * tok
    scratch = [
        v((3, blk, hid), BF16), v((3, blk, hid), BF16), v((fl, rows), BF16), v((fl, rows), BF16), v((rows, fl), BF16), v((rows, fl), BF16),
        v((fl, hid), BF16), v((fl, hid), BF16), v((fl, hid), BF16), v((tok, hid), BF16), v((1, hid), BF16),
        v((tok, hid), BF16), v((rows, ol), BF16), v((ol, hid), BF16),
        v((blk, fl), F32), v((2, blk, fl), BF16), v((2, blk, fl), BF16), v((blk, fl), BF16),
        v((2, 2 * tok, hid), BF16), v((2, 2 * tok, hid), BF16), v((2, 2 * tok, hid), BF16),
        v((2, tok, hid), BF16), v((3, tok, hid), BF16), v((tok, hid), F32),
        v((blk, ol), F32), v((blk, ol), BF16)]
    anyspec = pl.BlockSpec(memory_space=pl.ANY)
    return pl.pallas_call(
        functools.partial(kernel, side),
        out_shape=out_shape,
        in_specs=[anyspec] * 12,
        out_specs=tuple([pl.BlockSpec(memory_space=pltpu.VMEM)] * 6),
        scratch_shapes=scratch + sems,
        compiler_params=pltpu.CompilerParams(collective_id=0, has_side_effects=True, vmem_limit_bytes=45000000),
    )(*args)


def solution(mesh):
    token_spec = P(("dp", "tp"), None)
    split_cols = P("dp", "tp")
    weight_cols = P(None, "tp")
    weight_rows = P("tp", None)
    side = math.isqrt(mesh.shape["tp"] // 2)

    def local_backward(x_norm, grad_y, u_gate, u_up, w_gate, w_up, w_down, x_in, gamma, grad_res, attn_out, w_out):
        grad_sum, grad_attn, gw_gate, gw_up, gw_down, gw_out = mega(
            side, x_norm, grad_y, u_gate.T, u_up.T, w_gate.T, w_up.T, w_down, x_in, gamma.reshape(1, -1),
            grad_res, attn_out, w_out)
        return grad_sum, grad_attn, gw_gate.T, gw_up.T, gw_down, gw_out

    return jax.shard_map(
        local_backward,
        mesh=mesh,
        in_specs=(token_spec, token_spec, split_cols, split_cols, weight_cols, weight_cols, weight_rows,
                  token_spec, P(None), token_spec, split_cols, weight_rows),
        out_specs=(token_spec, split_cols, split_cols, split_cols, token_spec, token_spec),
        check_vma=False,
    )
```

```python
import functools
import math

import jax
import jax.numpy as jnp
from jax import lax
from jax.experimental import pallas as pl
from jax.experimental.pallas import tpu as pltpu
from jax.sharding import PartitionSpec as P

NORM_EPS = 1e-5
F32, BF16 = jnp.float32, jnp.bfloat16
LAG_R = 3
PIECES = 2
X_PIECES = 4
SUBS = 4
SLOTS = 6
NN = (((1,), (0,)), ((), ()))
NT = (((1,), (1,)), ((), ()))
TN = (((0,), (0,)), ((), ()))


def dot(a, b, dims):
    return lax.dot_general(a, b, dims, preferred_element_type=F32)


def kernel(side, x_in_hbm, gy_in_hbm, ug_hbm, uu_hbm, wg_hbm, wu_hbm, wd_hbm, xin_hbm, gamma_hbm, gr_hbm, o_hbm, wo_hbm,
           ds_out, do_v, acc_g, acc_u, acc_d, acc_o,
           yb, xb, ugt, uut, ug, uu, wg, wu, wd, xin, gamma, gr, ov, wo,
           g_s, g_t, du_g, du_u, z_s, own_part, pp_send, pp_recv, rs_send, rs_recv, acc0,
           do_acc, o_pair,
           y_rs, y_rr, y_ps, y_pr, x_rs, x_rr, x_ps, x_pr,
           s_rs, s_rr, s_ps, s_pr, r_s, r_r, q_s, q_r, loc):
    n = side * side
    tok, hid = x_in_hbm.shape
    half = tok // 2
    ct = hid // 8

    me = lax.axis_index("tp")
    core = me % 2
    chip = me // 2
    cy, cx = chip // side, chip % side
    diag = (cx + cy) % side
    pos_own = side * (cy * (1 - core) + cx * core) + diag
    pos_par = side * (cx * (1 - core) + cy * core) + diag

    def index_of(e, q):
        a, b = q // side, q % side
        o = (b - a + side) % side
        yy = a * (1 - e) + o * e
        xx = o * (1 - e) + a * e
        return (yy * side + xx) * 2 + e

    partner = me + 1 - 2 * core
    nxt = (index_of(core, (pos_own + 1) % n), index_of(core, (pos_own + n - 1) % n))

    def token_row(s, rel, d):
        e = core if rel == 0 else 1 - core
        base = pos_own if rel == 0 else pos_par
        q = (base + n - s) % n if d == 0 else (base + s) % n
        return pl.multiple_of(index_of(e, q) * tok + half * d, half)

    def remote(src, dst, ssem, rsem, dev):
        return pltpu.make_async_remote_copy(src_ref=src, dst_ref=dst, send_sem=ssem, recv_sem=rsem,
                                            device_id={"tp": dev}, device_id_type=pl.DeviceIdType.MESH)

    def local(i):
        pairs = ((gy_in_hbm, yb.at[0, pl.ds(0, tok), :]), (x_in_hbm, xb.at[0, pl.ds(0, tok), :]),
                 (wd_hbm, wd), (ug_hbm, ugt), (uu_hbm, uut), (wg_hbm, wg), (wu_hbm, wu),
                 (xin_hbm, xin), (gamma_hbm, gamma), (gr_hbm, gr), (o_hbm, ov), (wo_hbm, wo))
        return pltpu.make_async_copy(pairs[i][0], pairs[i][1], loc.at[i])

    for i in range(12):
        local(i).start()

    barrier = pltpu.get_barrier_semaphore()
    for dev in (nxt[0], nxt[1], partner):
        pl.semaphore_signal(barrier, inc=1, device_id={"tp": dev}, device_id_type=pl.DeviceIdType.MESH)
    pl.semaphore_wait(barrier, 3)

    def rows_at(s, rel, d):
        return pl.ds(pl.multiple_of((s % 2) * (2 * tok) + rel * tok + d * half, half), half)

    def cols_of(c, pieces):
        return pl.ds(c * (hid // pieces), hid // pieces)

    def ring_copy(b, sems, s, d, c, pieces):
        cols = cols_of(c, pieces)
        m = sems[0].shape[2]
        return remote(b.at[(s // 2) % 3, rows_at(s, 0, d), cols], b.at[((s + 1) // 2) % 3, rows_at(s + 1, 0, d), cols],
                      sems[0].at[d, c, s % m], sems[1].at[d, c, (s + 1) % m], nxt[d])

    def pair_copy(b, sems, s, d, c, pieces):
        cols = cols_of(c, pieces)
        m = sems[0].shape[2]
        return remote(b.at[(s // 2) % 3, rows_at(s, 0, d), cols], b.at[(s // 2) % 3, rows_at(s, 1, d), cols],
                      sems[2].at[d, c, s % m], sems[3].at[d, c, s % m], partner)

    def between(s, lo, hi):
        return jnp.logical_and(s >= lo, s <= hi)

    def each(pieces, f, part=None):
        for c in part or range(pieces):
            for d in range(2):
                f(d, c, pieces)

    def forward(b, sems, s, pieces, part=None):

        def one(d, c, pieces):
            @pl.when(between(s, 1, n - 1))
            def _():
                ring_copy(b, sems, s - 1, d, c, pieces).wait_recv()

            @pl.when(between(s, 0, n - 2))
            def _():
                ring_copy(b, sems, s, d, c, pieces).start()

            @pl.when(between(s, 0, n - 1))
            def _():
                pair_copy(b, sems, s, d, c, pieces).start()
        each(pieces, one, part)

        @pl.when(between(s, 2, n + 1))
        def _():
            each(pieces, lambda d, c, p: pair_copy(b, sems, s - 2, d, c, p).wait_send(), part)

        @pl.when(between(s, 2, n))
        def _():
            each(pieces, lambda d, c, p: ring_copy(b, sems, s - 2, d, c, p).wait_send(), part)

    def pair_wait(b, sems, s, pieces, part=None):
        each(pieces, lambda d, c, p: pair_copy(b, sems, s, d, c, p).wait_recv(), part)

    y_sems, x_sems, s_sems = (y_rs, y_rr, y_ps, y_pr), (x_rs, x_rr, x_ps, x_pr), (s_rs, s_rr, s_ps, s_pr)

    early, late = tuple(range(X_PIECES // 2)), tuple(range(X_PIECES // 2, X_PIECES))

    def part_a(t):
        @pl.when(t == 0)
        def _():
            local(0).wait()
        forward(yb, y_sems, t, PIECES)

    def part_b(t):
        @pl.when(t == 0)
        def _():
            local(1).wait()
        forward(xb, x_sems, t, X_PIECES, early)

    def part_c(s):
        forward(xb, x_sems, s, X_PIECES, late)

    def task_1(k):
        @pl.when(k == 0)
        def _():
            for i in (2, 3, 4):
                local(i).wait()

            def turn(c, carry):
                cols = pl.ds(pl.multiple_of(c * 128, 128), 128)
                ug[cols, :] = ugt[:, cols].astype(F32).T.astype(BF16)
                uu[cols, :] = uut[:, cols].astype(F32).T.astype(BF16)
                return carry
            lax.fori_loop(0, ug.shape[0] // 128, turn, 0)
        pair_wait(yb, y_sems, 2 * k, PIECES)
        pair_wait(yb, y_sems, 2 * k + 1, PIECES)
        g_t[...] = dot(wd[:, :hid // 2], yb[k % 3, :, :hid // 2], NT)

    def task_1b(k):
        g_s[...] = (g_t[...] + dot(wd[:, hid // 2:], yb[k % 3, :, hid // 2:], NT)).T
        for i in range(2):
            for rel in range(2):
                for d in range(2):
                    r0 = i * 2 * tok + rel * tok + d * half
                    row = token_row(2 * k + i, rel, d)
                    gate = ug[pl.ds(row, half), :].astype(F32)
                    up = uu[pl.ds(row, half), :].astype(F32)
                    sig = jax.nn.sigmoid(gate)
                    act = gate * sig
                    grad = g_s[pl.ds(r0, half), :]
                    z_s[pl.ds(r0, half), :] = (act * up).astype(BF16)
                    du_u[k, pl.ds(r0, half), :] = (grad * act).astype(BF16)
                    du_g[k, pl.ds(r0, half), :] = (grad * up * (sig * (1.0 + gate * (1.0 - sig)))).astype(BF16)

    def pp_copy(k):
        return remote(pp_send.at[k % 2], pp_recv.at[k % 2], q_s.at[k % 2], q_r.at[k % 2], partner)

    def task_2(k, lo, hi):
        ks = k % 2
        if lo == 0:
            @pl.when(k == 0)
            def _():
                local(5).wait()
                local(6).wait()

            @pl.when(k >= 2)
            def _():
                pp_copy(k - 2).wait_send()

        def body(c, carry):
            cols = pl.ds(pl.multiple_of(c * ct, ct), ct)
            r = (dot(du_g[k], wg[:, cols], NN) + dot(du_u[k], wu[:, cols], NN)).astype(BF16)
            for i in range(2):
                own_part[ks, pl.ds(i * tok, tok), cols] = r[i * 2 * tok:i * 2 * tok + tok]
                pp_send[ks, pl.ds(i * tok, tok), cols] = r[i * 2 * tok + tok:(i + 1) * 2 * tok]
            return carry
        lax.fori_loop(lo, hi, body, 0)
        if hi == 8:
            pp_copy(k).start()

    def task_3(k):
        def body(c, carry):
            cols = pl.ds(pl.multiple_of(c * ct, ct), ct)
            acc_d[:, cols] += dot(z_s[...], yb[k % 3, :, cols], TN)
            return carry
        lax.fori_loop(0, 8, body, 0)

    def task_4(k, lo, hi):
        if lo in (0, 4):
            part = early if lo == 0 else late
            pair_wait(xb, x_sems, 2 * k, X_PIECES, part)
            pair_wait(xb, x_sems, 2 * k + 1, X_PIECES, part)

        def body(c, carry):
            cols = pl.ds(pl.multiple_of(c * ct, ct), ct)
            xt = xb[k % 3, :, cols]
            acc_g[:, cols] += dot(du_g[k], xt, TN)
            acc_u[:, cols] += dot(du_u[k], xt, TN)
            return carry
        lax.fori_loop(lo, hi, body, 0)

    def rs_copy(j, d, c, pieces):
        rows, cols = pl.ds(d * half, half), cols_of(c, pieces)
        return remote(rs_send.at[j % 2, rows, cols], rs_recv.at[(j + 1) % 3, rows, cols],
                      r_s.at[d, c, j % 2], r_r.at[d, c, (j + 1) % 3], nxt[d])

    def part_d(t, i):
        j = t - LAG_R
        ks = (j // 2) % 2
        rows = pl.ds(i * tok, tok)
        if i == 0:
            @pl.when(between(j, 0, n - 2))
            def _():
                pp_copy(j // 2).wait_recv()

            @pl.when(j == 0)
            def _():
                acc0[...] = own_part[ks, rows, :].astype(F32) + pp_recv[ks, rows, :].astype(F32)

        @pl.when(between(j, 3, n + 1))
        def _():
            each(PIECES, lambda d, c, p: rs_copy(j - 2, d, c, p).wait_send())

        def one(d, c, pieces):
            dr = pl.ds(d * half, half)
            pr = pl.ds(i * tok + d * half, half)
            cols = cols_of(c, pieces)

            @pl.when(between(j, 2, n))
            def _():
                rs_copy(j - 1, d, c, pieces).wait_recv()

            @pl.when(j == 1)
            def _():
                rs_send[j % 2, dr, cols] = (own_part[ks, pr, cols].astype(F32)
                                            + pp_recv[ks, pr, cols].astype(F32)).astype(BF16)

            @pl.when(between(j, 2, n - 1))
            def _():
                rs_send[j % 2, dr, cols] = (own_part[ks, pr, cols].astype(F32) + pp_recv[ks, pr, cols].astype(F32)
                                            + rs_recv[j % 3, dr, cols].astype(F32)).astype(BF16)

            @pl.when(between(j, 1, n - 1))
            def _():
                rs_copy(j, d, c, pieces).start()
        each(PIECES, one)

    def pair_body(kk, carry):
        t = 2 * kk
        part_a(t)

        @pl.when(kk == 0)
        def _():
            part_b(t)
            acc_d[...] = jnp.zeros_like(acc_d)
            acc_g[...] = jnp.zeros_like(acc_g)
            acc_u[...] = jnp.zeros_like(acc_u)
            acc_o[...] = jnp.zeros_like(acc_o)

        @pl.when(kk >= 1)
        def _():
            task_2(kk - 1, 0, 4)
            part_d(t, 1)
            task_2(kk - 1, 4, 8)
            part_b(t)
            task_4(kk - 1, 0, 4)

        @pl.when(kk == n // 2)
        def _():
            part_c(t - n)
        t = 2 * kk + 1
        part_a(t)

        @pl.when(kk >= 1)
        def _():
            task_3(kk - 1)
            part_d(t, 0)

        @pl.when(kk < n // 2)
        def _():
            task_1(kk)
        part_b(t)

        @pl.when(kk < n // 2)
        def _():
            task_1b(kk)

        @pl.when(kk == n // 2)
        def _():
            part_c(t - n)
        return carry

    lax.fori_loop(0, n // 2 + 1, pair_body, 0)
    part_d(jnp.int32(n + 2), 1)
    part_c(jnp.int32(2))
    part_d(jnp.int32(n + 3), 0)

    for i in (7, 8, 9, 10, 11):
        local(i).wait()

    def norm(c, carry):
        rows = pl.ds(pl.multiple_of(c * 16, 16), 16)
        xf = xin[rows, :].astype(F32)
        inv = lax.rsqrt(jnp.mean(xf * xf, axis=-1, keepdims=True) + NORM_EPS)
        gx = (acc0[rows, :] + rs_recv[n % 3, rows, :].astype(F32)).astype(BF16)
        scaled = gx.astype(F32) * gamma[...].astype(F32).reshape(1, hid)
        proj = jnp.mean(scaled * xf, axis=-1, keepdims=True)
        ds = (gr[rows, :].astype(F32) + inv * (scaled - xf * (inv * inv) * proj)).astype(BF16)
        yb[0, rows, :] = ds
        ds_out[rows, :] = ds
        return carry
    lax.fori_loop(0, tok // 16, norm, 0)

    def o_task(m, c):
        cols = pl.ds(pl.multiple_of(c * ct, ct), ct)
        blk = yb[m % 3, :, cols]
        acc_o[:, cols] += dot(o_pair[...], blk, TN)
        part = dot(blk, wo[:, cols], NT)

        @pl.when(c == 0)
        def _():
            do_acc[...] = part

        @pl.when(c > 0)
        def _():
            do_acc[...] += part

    def o_rows(m):
        for i in range(2):
            for rel in range(2):
                for d in range(2):
                    yield i * 2 * tok + rel * tok + d * half, token_row(2 * m + i, rel, d)

    def o_begin(m):
        for r0, row in o_rows(m):
            o_pair[pl.ds(r0, half), :] = ov[pl.ds(row, half), :]

    def o_end(m):
        for r0, row in o_rows(m):
            do_v[pl.ds(row, half), :] = do_acc[pl.ds(r0, half), :].astype(BF16)

    def s_step(u, carry):
        m = u // 2 - 1

        @pl.when(jnp.logical_and(u >= 2, u % 2 == 0))
        def _():
            each(SUBS, lambda d, c, p: pair_copy(yb, s_sems, 2 * m, d, c, p).wait_recv())
            each(SUBS, lambda d, c, p: pair_copy(yb, s_sems, 2 * m + 1, d, c, p).wait_recv())
            o_begin(m)
        for c in range(SUBS):
            for d in range(2):
                @pl.when(between(u, 1, n - 1))
                def _():
                    ring_copy(yb, s_sems, u - 1, d, c, SUBS).wait_recv()

                @pl.when(u <= n - 2)
                def _():
                    ring_copy(yb, s_sems, u, d, c, SUBS).start()

                @pl.when(u <= n - 1)
                def _():
                    pair_copy(yb, s_sems, u, d, c, SUBS).start()

                @pl.when(between(u, 2, n + 1))
                def _():
                    pair_copy(yb, s_sems, u - 2, d, c, SUBS).wait_send()

                @pl.when(between(u, 2, n))
                def _():
                    ring_copy(yb, s_sems, u - 2, d, c, SUBS).wait_send()

            if c % 2 == 1:
                forward(xb, x_sems, u + 3, X_PIECES, (late[c // 2],))

            @pl.when(u >= 2)
            def _():
                o_task(m, (u % 2) * SUBS + c)

        @pl.when(jnp.logical_and(u >= 2, u % 2 == 1))
        def _():
            o_end(m)

        @pl.when(u == 0)
        def _():
            task_4(0, 4, 8)

        @pl.when(jnp.logical_and(u <= n - 2, u % 2 == 1))
        def _():
            task_4((u + 1) // 2, 4, 6)

        @pl.when(jnp.logical_and(between(u, 2, n - 2), u % 2 == 0))
        def _():
            task_4(u // 2, 6, 8)
        return carry

    lax.fori_loop(0, n + 2, s_step, 0)
    each(PIECES, lambda d, c, p: rs_copy(n - 1, d, c, p).wait_send())
    pp_copy(n // 2 - 2).wait_send()
    pp_copy(n // 2 - 1).wait_send()


def mega(side, *args):
    tok, hid = args[0].shape
    fl, rows = args[2].shape
    ol = args[10].shape[1]
    dma = pltpu.SemaphoreType.DMA
    ring = [dma((2, PIECES, SLOTS)) for _ in range(4)] + [dma((2, X_PIECES, SLOTS)) for _ in range(4)] + [dma((2, SUBS, 4)) for _ in range(4)]
    sems = ring + [dma((2, PIECES, 2)), dma((2, PIECES, 3)), dma((2,)), dma((2,)), dma((12,))]
    out_shape = (pltpu.VMEM((tok, hid), BF16), pltpu.VMEM((rows, ol), BF16), pltpu.VMEM((fl, hid), F32),
                 pltpu.VMEM((fl, hid), F32), pltpu.VMEM((fl, hid), F32), pltpu.VMEM((ol, hid), F32))
    v = pltpu.VMEM
    blk = 4 * tok
    scratch = [
        v((3, blk, hid), BF16), v((3, blk, hid), BF16), v((fl, rows), BF16), v((fl, rows), BF16), v((rows, fl), BF16), v((rows, fl), BF16),
        v((fl, hid), BF16), v((fl, hid), BF16), v((fl, hid), BF16), v((tok, hid), BF16), v((hid,), BF16),
        v((tok, hid), BF16), v((rows, ol), BF16), v((ol, hid), BF16),
        v((blk, fl), F32), v((fl, blk), F32), v((rows // blk, blk, fl), BF16), v((rows // blk, blk, fl), BF16), v((blk, fl), BF16),
        v((2, 2 * tok, hid), BF16), v((2, 2 * tok, hid), BF16), v((2, 2 * tok, hid), BF16),
        v((2, tok, hid), BF16), v((3, tok, hid), BF16), v((tok, hid), F32),
        v((blk, ol), F32), v((blk, ol), BF16)]
    anyspec = pl.BlockSpec(memory_space=pl.ANY)
    return pl.pallas_call(
        functools.partial(kernel, side),
        out_shape=out_shape,
        in_specs=[anyspec] * 12,
        out_specs=tuple([pl.BlockSpec(memory_space=pltpu.VMEM)] * 6),
        scratch_shapes=scratch + sems,
        compiler_params=pltpu.CompilerParams(collective_id=0, has_side_effects=True, vmem_limit_bytes=46800000),
    )(*args)


def flush_kernel(*refs):
    k = len(refs) // 2
    copies = [pltpu.make_async_copy(refs[i], refs[k + i], refs[-1].at[i]) for i in range(k)]
    for c in copies:
        c.start()
    for c in copies:
        c.wait()


def flush(*arrays):
    return pl.pallas_call(
        flush_kernel,
        out_shape=tuple(pltpu.HBM(a.shape, a.dtype) for a in arrays),
        in_specs=[pl.BlockSpec(memory_space=pltpu.VMEM)] * len(arrays),
        out_specs=tuple([pl.BlockSpec(memory_space=pltpu.HBM)] * len(arrays)),
        scratch_shapes=[pltpu.SemaphoreType.DMA((len(arrays),))],
        compiler_params=pltpu.CompilerParams(vmem_limit_bytes=1000000),
    )(*[pltpu.with_memory_space_constraint(a, pltpu.VMEM) for a in arrays])


def solution(mesh):
    token_spec = P(("dp", "tp"), None)
    split_cols = P("dp", "tp")
    weight_cols = P(None, "tp")
    weight_rows = P("tp", None)
    side = math.isqrt(mesh.shape["tp"] // 2)

    def local_backward(x_norm, grad_y, u_gate, u_up, w_gate, w_up, w_down, x_in, gamma, grad_res, attn_out, w_out):
        grad_sum, grad_attn, gw_gate, gw_up, gw_down, gw_out = flush(*mega(
            side, x_norm, grad_y, u_gate.T, u_up.T, w_gate.T, w_up.T, w_down, x_in, gamma,
            grad_res, attn_out, w_out))
        return grad_sum, grad_attn, gw_gate.T, gw_up.T, gw_down, gw_out

    return jax.shard_map(
        local_backward,
        mesh=mesh,
        in_specs=(token_spec, token_spec, split_cols, split_cols, weight_cols, weight_cols, weight_rows,
                  token_spec, P(None), token_spec, split_cols, weight_rows),
        out_specs=(token_spec, split_cols, split_cols, split_cols, token_spec, token_spec),
        check_vma=False,
    )
```

```python
import functools
import math

import jax
import jax.numpy as jnp
from jax import lax
from jax.experimental import pallas as pl
from jax.experimental.pallas import tpu as pltpu
from jax.sharding import PartitionSpec as P

NORM_EPS = 1e-5
F32, BF16 = jnp.float32, jnp.bfloat16
LAG_R = 3
PIECES = 2
X_PIECES = 4
TILES = 4
SUBS = 4
SLOTS = 6
NN = (((1,), (0,)), ((), ()))
NT = (((1,), (1,)), ((), ()))
TN = (((0,), (0,)), ((), ()))


def dot(a, b, dims):
    return lax.dot_general(a, b, dims, preferred_element_type=F32)


def kernel(side, x_in_hbm, gy_in_hbm, ug_hbm, uu_hbm, wg_hbm, wu_hbm, wd_hbm, xin_hbm, gamma_hbm, gr_hbm, o_hbm, wo_hbm,
           ds_out, do_v, acc_g, acc_u, acc_d, acc_o,
           yb, xb, ugt, uut, ug, uu, wg, wu, wd, xin, gamma, gr, ov, wo,
           g_s, du_g, du_u, z_s, own_part, pp_send, pp_recv, rs_send, rs_recv, acc0,
           do_acc, o_pair,
           y_rs, y_rr, y_ps, y_pr, x_rs, x_rr, x_ps, x_pr,
           s_rs, s_rr, s_ps, s_pr, r_s, r_r, q_s, q_r, loc):
    n = side * side
    tok, hid = x_in_hbm.shape
    half = tok // 2
    ct = hid // TILES

    me = lax.axis_index("tp")
    core = me % 2
    chip = me // 2
    cy, cx = chip // side, chip % side
    diag = (cx + cy) % side
    pos_own = side * (cy * (1 - core) + cx * core) + diag
    pos_par = side * (cx * (1 - core) + cy * core) + diag

    def index_of(e, q):
        a, b = q // side, q % side
        o = (b - a + side) % side
        yy = a * (1 - e) + o * e
        xx = o * (1 - e) + a * e
        return (yy * side + xx) * 2 + e

    partner = me + 1 - 2 * core
    nxt = (index_of(core, (pos_own + 1) % n), index_of(core, (pos_own + n - 1) % n))

    def token_row(s, rel, d):
        e = core if rel == 0 else 1 - core
        base = pos_own if rel == 0 else pos_par
        q = (base + n - s) % n if d == 0 else (base + s) % n
        return pl.multiple_of(index_of(e, q) * tok + half * d, half)

    def remote(src, dst, ssem, rsem, dev):
        return pltpu.make_async_remote_copy(src_ref=src, dst_ref=dst, send_sem=ssem, recv_sem=rsem,
                                            device_id={"tp": dev}, device_id_type=pl.DeviceIdType.MESH)

    def local(i):
        pairs = ((gy_in_hbm, yb.at[0, pl.ds(0, tok), :]), (x_in_hbm, xb.at[0, pl.ds(0, tok), :]),
                 (wd_hbm, wd), (ug_hbm, ugt), (uu_hbm, uut), (wg_hbm, wg), (wu_hbm, wu),
                 (xin_hbm, xin), (gamma_hbm, gamma), (gr_hbm, gr), (o_hbm, ov), (wo_hbm, wo))
        return pltpu.make_async_copy(pairs[i][0], pairs[i][1], loc.at[i])

    for i in range(12):
        local(i).start()

    barrier = pltpu.get_barrier_semaphore()
    for dev in (nxt[0], nxt[1], partner):
        pl.semaphore_signal(barrier, inc=1, device_id={"tp": dev}, device_id_type=pl.DeviceIdType.MESH)
    pl.semaphore_wait(barrier, 3)

    def rows_at(s, rel, d):
        return pl.ds(pl.multiple_of((s % 2) * (2 * tok) + rel * tok + d * half, half), half)

    def cols_of(c, pieces):
        return pl.ds(c * (hid // pieces), hid // pieces)

    def ring_copy(b, sems, s, d, c, pieces):
        cols = cols_of(c, pieces)
        m = sems[0].shape[2]
        return remote(b.at[(s // 2) % 3, rows_at(s, 0, d), cols], b.at[((s + 1) // 2) % 3, rows_at(s + 1, 0, d), cols],
                      sems[0].at[d, c, s % m], sems[1].at[d, c, (s + 1) % m], nxt[d])

    def pair_copy(b, sems, s, d, c, pieces):
        cols = cols_of(c, pieces)
        m = sems[0].shape[2]
        return remote(b.at[(s // 2) % 3, rows_at(s, 0, d), cols], b.at[(s // 2) % 3, rows_at(s, 1, d), cols],
                      sems[2].at[d, c, s % m], sems[3].at[d, c, s % m], partner)

    def between(s, lo, hi):
        return jnp.logical_and(s >= lo, s <= hi)

    def each(pieces, f, part=None):
        for c in part or range(pieces):
            for d in range(2):
                f(d, c, pieces)

    def forward(b, sems, s, pieces, part=None):

        def one(d, c, pieces):
            @pl.when(between(s, 1, n - 1))
            def _():
                ring_copy(b, sems, s - 1, d, c, pieces).wait_recv()

            @pl.when(between(s, 0, n - 2))
            def _():
                ring_copy(b, sems, s, d, c, pieces).start()

            @pl.when(between(s, 0, n - 1))
            def _():
                pair_copy(b, sems, s, d, c, pieces).start()
        each(pieces, one, part)

        @pl.when(between(s, 2, n + 1))
        def _():
            each(pieces, lambda d, c, p: pair_copy(b, sems, s - 2, d, c, p).wait_send(), part)

        @pl.when(between(s, 2, n))
        def _():
            each(pieces, lambda d, c, p: ring_copy(b, sems, s - 2, d, c, p).wait_send(), part)

    def pair_wait(b, sems, s, pieces, part=None):
        each(pieces, lambda d, c, p: pair_copy(b, sems, s, d, c, p).wait_recv(), part)

    y_sems, x_sems, s_sems = (y_rs, y_rr, y_ps, y_pr), (x_rs, x_rr, x_ps, x_pr), (s_rs, s_rr, s_ps, s_pr)

    early, late = tuple(range(X_PIECES // 2)), tuple(range(X_PIECES // 2, X_PIECES))

    def part_a(t):
        @pl.when(t == 0)
        def _():
            local(0).wait()
        forward(yb, y_sems, t, PIECES)

    def part_b(t):
        @pl.when(t == 0)
        def _():
            local(1).wait()
        forward(xb, x_sems, t, X_PIECES, early)

    def part_c(s):
        forward(xb, x_sems, s, X_PIECES, late)

    def task_1(k):
        @pl.when(k == 0)
        def _():
            for i in (2, 3, 4):
                local(i).wait()

            def turn(c, carry):
                cols = pl.ds(pl.multiple_of(c * 128, 128), 128)
                ug[cols, :] = ugt[:, cols].astype(F32).T.astype(BF16)
                uu[cols, :] = uut[:, cols].astype(F32).T.astype(BF16)
                return carry
            lax.fori_loop(0, ug.shape[0] // 128, turn, 0)
        pair_wait(yb, y_sems, 2 * k, PIECES)
        pair_wait(yb, y_sems, 2 * k + 1, PIECES)

    def task_1b(k):
        g_s[...] = dot(wd[...], yb[k % 3], NT).T
        for i in range(2):
            for rel in range(2):
                for d in range(2):
                    r0 = i * 2 * tok + rel * tok + d * half
                    row = token_row(2 * k + i, rel, d)
                    gate = ug[pl.ds(row, half), :].astype(F32)
                    up = uu[pl.ds(row, half), :].astype(F32)
                    sig = jax.nn.sigmoid(gate)
                    act = gate * sig
                    grad = g_s[pl.ds(r0, half), :]
                    z_s[pl.ds(r0, half), :] = (act * up).astype(BF16)
                    du_u[k, pl.ds(r0, half), :] = (grad * act).astype(BF16)
                    du_g[k, pl.ds(r0, half), :] = (grad * up * (sig * (1.0 + gate * (1.0 - sig)))).astype(BF16)

    def pp_copy(k):
        return remote(pp_send.at[k % 2], pp_recv.at[k % 2], q_s.at[k % 2], q_r.at[k % 2], partner)

    def task_2(k, lo, hi):
        ks = k % 2
        if lo == 0:
            @pl.when(k == 0)
            def _():
                local(5).wait()
                local(6).wait()

            @pl.when(k >= 2)
            def _():
                pp_copy(k - 2).wait_send()

        def body(c, carry):
            cols = pl.ds(pl.multiple_of(c * ct, ct), ct)
            r = (dot(du_g[k], wg[:, cols], NN) + dot(du_u[k], wu[:, cols], NN)).astype(BF16)
            for i in range(2):
                own_part[ks, pl.ds(i * tok, tok), cols] = r[i * 2 * tok:i * 2 * tok + tok]
                pp_send[ks, pl.ds(i * tok, tok), cols] = r[i * 2 * tok + tok:(i + 1) * 2 * tok]
            return carry
        lax.fori_loop(lo, hi, body, 0)
        if hi == TILES:
            pp_copy(k).start()

    def task_3(k):
        def body(c, carry):
            cols = pl.ds(pl.multiple_of(c * ct, ct), ct)
            acc_d[:, cols] += dot(z_s[...], yb[k % 3, :, cols], TN)
            return carry
        lax.fori_loop(0, TILES, body, 0)

    def task_4(k, lo, hi):
        if lo in (0, TILES // 2):
            part = early if lo == 0 else late
            pair_wait(xb, x_sems, 2 * k, X_PIECES, part)
            pair_wait(xb, x_sems, 2 * k + 1, X_PIECES, part)

        def body(c, carry):
            cols = pl.ds(pl.multiple_of(c * ct, ct), ct)
            xt = xb[k % 3, :, cols]
            acc_g[:, cols] += dot(du_g[k], xt, TN)
            acc_u[:, cols] += dot(du_u[k], xt, TN)
            return carry
        lax.fori_loop(lo, hi, body, 0)

    def rs_copy(j, d, c, pieces):
        rows, cols = pl.ds(d * half, half), cols_of(c, pieces)
        return remote(rs_send.at[j % 2, rows, cols], rs_recv.at[(j + 1) % 3, rows, cols],
                      r_s.at[d, c, j % 2], r_r.at[d, c, (j + 1) % 3], nxt[d])

    def part_d(t, i):
        j = t - LAG_R
        ks = (j // 2) % 2
        rows = pl.ds(i * tok, tok)
        if i == 0:
            @pl.when(between(j, 0, n - 2))
            def _():
                pp_copy(j // 2).wait_recv()

            @pl.when(j == 0)
            def _():
                acc0[...] = own_part[ks, rows, :].astype(F32) + pp_recv[ks, rows, :].astype(F32)

        @pl.when(between(j, 3, n + 1))
        def _():
            each(PIECES, lambda d, c, p: rs_copy(j - 2, d, c, p).wait_send())

        def one(d, c, pieces):
            dr = pl.ds(d * half, half)
            pr = pl.ds(i * tok + d * half, half)
            cols = cols_of(c, pieces)

            @pl.when(between(j, 2, n))
            def _():
                rs_copy(j - 1, d, c, pieces).wait_recv()

            @pl.when(j == 1)
            def _():
                rs_send[j % 2, dr, cols] = (own_part[ks, pr, cols].astype(F32)
                                            + pp_recv[ks, pr, cols].astype(F32)).astype(BF16)

            @pl.when(between(j, 2, n - 1))
            def _():
                rs_send[j % 2, dr, cols] = (own_part[ks, pr, cols].astype(F32) + pp_recv[ks, pr, cols].astype(F32)
                                            + rs_recv[j % 3, dr, cols].astype(F32)).astype(BF16)

            @pl.when(between(j, 1, n - 1))
            def _():
                rs_copy(j, d, c, pieces).start()
        each(PIECES, one)

    def pair_body(kk, carry):
        t = 2 * kk
        part_a(t)

        @pl.when(kk == 0)
        def _():
            part_b(t)
            acc_d[...] = jnp.zeros_like(acc_d)
            acc_g[...] = jnp.zeros_like(acc_g)
            acc_u[...] = jnp.zeros_like(acc_u)
            acc_o[...] = jnp.zeros_like(acc_o)

        @pl.when(kk >= 1)
        def _():
            task_2(kk - 1, 0, TILES // 2)
            part_d(t, 1)
            task_2(kk - 1, TILES // 2, TILES)
            part_b(t)
            task_4(kk - 1, 0, TILES // 2)

        @pl.when(kk == n // 2)
        def _():
            part_c(t - n)
        t = 2 * kk + 1
        part_a(t)

        @pl.when(kk >= 1)
        def _():
            task_3(kk - 1)
            part_d(t, 0)

        @pl.when(kk < n // 2)
        def _():
            task_1(kk)
        part_b(t)

        @pl.when(kk < n // 2)
        def _():
            task_1b(kk)

        @pl.when(kk == n // 2)
        def _():
            part_c(t - n)
        return carry

    lax.fori_loop(0, n // 2 + 1, pair_body, 0)
    part_d(jnp.int32(n + 2), 1)
    part_c(jnp.int32(2))
    part_d(jnp.int32(n + 3), 0)

    for i in (7, 8, 9, 10, 11):
        local(i).wait()

    def norm(c, carry):
        rows = pl.ds(pl.multiple_of(c * 16, 16), 16)
        xf = xin[rows, :].astype(F32)
        inv = lax.rsqrt(jnp.mean(xf * xf, axis=-1, keepdims=True) + NORM_EPS)
        gx = (acc0[rows, :] + rs_recv[n % 3, rows, :].astype(F32)).astype(BF16)
        scaled = gx.astype(F32) * gamma[...].astype(F32).reshape(1, hid)
        proj = jnp.mean(scaled * xf, axis=-1, keepdims=True)
        ds = (gr[rows, :].astype(F32) + inv * (scaled - xf * (inv * inv) * proj)).astype(BF16)
        yb[0, rows, :] = ds
        ds_out[rows, :] = ds
        return carry
    lax.fori_loop(0, tok // 16, norm, 0)

    def o_task(m, c):
        cols = pl.ds(pl.multiple_of(c * ct, ct), ct)
        blk = yb[m % 3, :, cols]
        acc_o[:, cols] += dot(o_pair[...], blk, TN)
        part = dot(blk, wo[:, cols], NT)

        @pl.when(c == 0)
        def _():
            do_acc[...] = part

        @pl.when(c > 0)
        def _():
            do_acc[...] += part

    def o_rows(m):
        for i in range(2):
            for rel in range(2):
                for d in range(2):
                    yield i * 2 * tok + rel * tok + d * half, token_row(2 * m + i, rel, d)

    def o_begin(m):
        for r0, row in o_rows(m):
            o_pair[pl.ds(r0, half), :] = ov[pl.ds(row, half), :]

    def o_end(m):
        for r0, row in o_rows(m):
            do_v[pl.ds(row, half), :] = do_acc[pl.ds(r0, half), :].astype(BF16)

    def s_step(u, carry):
        m = u // 2 - 1

        @pl.when(jnp.logical_and(u >= 2, u % 2 == 0))
        def _():
            each(SUBS, lambda d, c, p: pair_copy(yb, s_sems, 2 * m, d, c, p).wait_recv())
            each(SUBS, lambda d, c, p: pair_copy(yb, s_sems, 2 * m + 1, d, c, p).wait_recv())
            o_begin(m)
        for c in range(SUBS):
            for d in range(2):
                @pl.when(between(u, 1, n - 1))
                def _():
                    ring_copy(yb, s_sems, u - 1, d, c, SUBS).wait_recv()

                @pl.when(u <= n - 2)
                def _():
                    ring_copy(yb, s_sems, u, d, c, SUBS).start()

                @pl.when(u <= n - 1)
                def _():
                    pair_copy(yb, s_sems, u, d, c, SUBS).start()

                @pl.when(between(u, 2, n + 1))
                def _():
                    pair_copy(yb, s_sems, u - 2, d, c, SUBS).wait_send()

                @pl.when(between(u, 2, n))
                def _():
                    ring_copy(yb, s_sems, u - 2, d, c, SUBS).wait_send()

            if c % 2 == 1:
                forward(xb, x_sems, u + 3, X_PIECES, (late[c // 2],))

            if c % (2 * SUBS // TILES) == 0:
                @pl.when(u >= 2)
                def _():
                    o_task(m, (u % 2) * (TILES // 2) + c * TILES // (2 * SUBS))

        @pl.when(jnp.logical_and(u >= 2, u % 2 == 1))
        def _():
            o_end(m)

        @pl.when(u == 0)
        def _():
            task_4(0, TILES // 2, TILES)

        @pl.when(jnp.logical_and(u <= n - 2, u % 2 == 1))
        def _():
            task_4((u + 1) // 2, TILES // 2, TILES)

        return carry

    lax.fori_loop(0, n + 2, s_step, 0)
    each(PIECES, lambda d, c, p: rs_copy(n - 1, d, c, p).wait_send())
    pp_copy(n // 2 - 2).wait_send()
    pp_copy(n // 2 - 1).wait_send()


def mega(side, *args):
    tok, hid = args[0].shape
    fl, rows = args[2].shape
    ol = args[10].shape[1]
    dma = pltpu.SemaphoreType.DMA
    ring = [dma((2, PIECES, SLOTS)) for _ in range(4)] + [dma((2, X_PIECES, SLOTS)) for _ in range(4)] + [dma((2, SUBS, 4)) for _ in range(4)]
    sems = ring + [dma((2, PIECES, 2)), dma((2, PIECES, 3)), dma((2,)), dma((2,)), dma((12,))]
    out_shape = (pltpu.VMEM((tok, hid), BF16), pltpu.VMEM((rows, ol), BF16), pltpu.VMEM((fl, hid), F32),
                 pltpu.VMEM((fl, hid), F32), pltpu.VMEM((fl, hid), F32), pltpu.VMEM((ol, hid), F32))
    v = pltpu.VMEM
    blk = 4 * tok
    scratch = [
        v((3, blk, hid), BF16), v((3, blk, hid), BF16), v((fl, rows), BF16), v((fl, rows), BF16), v((rows, fl), BF16), v((rows, fl), BF16),
        v((fl, hid), BF16), v((fl, hid), BF16), v((fl, hid), BF16), v((tok, hid), BF16), v((hid,), BF16),
        v((tok, hid), BF16), v((rows, ol), BF16), v((ol, hid), BF16),
        v((blk, fl), F32), v((rows // blk, blk, fl), BF16), v((rows // blk, blk, fl), BF16), v((blk, fl), BF16),
        v((2, 2 * tok, hid), BF16), v((2, 2 * tok, hid), BF16), v((2, 2 * tok, hid), BF16),
        v((2, tok, hid), BF16), v((3, tok, hid), BF16), v((tok, hid), F32),
        v((blk, ol), F32), v((blk, ol), BF16)]
    anyspec = pl.BlockSpec(memory_space=pl.ANY)
    return pl.pallas_call(
        functools.partial(kernel, side),
        out_shape=out_shape,
        in_specs=[anyspec] * 12,
        out_specs=tuple([pl.BlockSpec(memory_space=pltpu.VMEM)] * 6),
        scratch_shapes=scratch + sems,
        compiler_params=pltpu.CompilerParams(collective_id=0, has_side_effects=True, vmem_limit_bytes=46800000),
    )(*args)


def flush_kernel(*refs):
    k = len(refs) // 2
    copies = [pltpu.make_async_copy(refs[i], refs[k + i], refs[-1].at[i]) for i in range(k)]
    for c in copies:
        c.start()
    for c in copies:
        c.wait()


def flush(*arrays):
    return pl.pallas_call(
        flush_kernel,
        out_shape=tuple(pltpu.HBM(a.shape, a.dtype) for a in arrays),
        in_specs=[pl.BlockSpec(memory_space=pltpu.VMEM)] * len(arrays),
        out_specs=tuple([pl.BlockSpec(memory_space=pltpu.HBM)] * len(arrays)),
        scratch_shapes=[pltpu.SemaphoreType.DMA((len(arrays),))],
        compiler_params=pltpu.CompilerParams(vmem_limit_bytes=1000000),
    )(*[pltpu.with_memory_space_constraint(a, pltpu.VMEM) for a in arrays])


def solution(mesh):
    token_spec = P(("dp", "tp"), None)
    split_cols = P("dp", "tp")
    weight_cols = P(None, "tp")
    weight_rows = P("tp", None)
    side = math.isqrt(mesh.shape["tp"] // 2)

    def local_backward(x_norm, grad_y, u_gate, u_up, w_gate, w_up, w_down, x_in, gamma, grad_res, attn_out, w_out):
        grad_sum, grad_attn, gw_gate, gw_up, gw_down, gw_out = flush(*mega(
            side, x_norm, grad_y, u_gate.T, u_up.T, w_gate.T, w_up.T, w_down, x_in, gamma,
            grad_res, attn_out, w_out))
        return grad_sum, grad_attn, gw_gate.T, gw_up.T, gw_down, gw_out

    return jax.shard_map(
        local_backward,
        mesh=mesh,
        in_specs=(token_spec, token_spec, split_cols, split_cols, weight_cols, weight_cols, weight_rows,
                  token_spec, P(None), token_spec, split_cols, weight_rows),
        out_specs=(token_spec, split_cols, split_cols, split_cols, token_spec, token_spec),
        check_vma=False,
    )
```

```python
import functools
import math

import jax
import jax.numpy as jnp
from jax import lax
from jax.experimental import pallas as pl
from jax.experimental.pallas import tpu as pltpu
from jax.sharding import PartitionSpec as P

NORM_EPS = 1e-5
F32, BF16 = jnp.float32, jnp.bfloat16
LAG_R = 3
PIECES = 2
X_PIECES = 4
TILES = 4
SUBS = 4
MEGA_VMEM = 39000000
FLUSH_VMEM = 4000000
SLOTS = 6
NN = (((1,), (0,)), ((), ()))
NT = (((1,), (1,)), ((), ()))
TN = (((0,), (0,)), ((), ()))


def dot(a, b, dims):
    return lax.dot_general(a, b, dims, preferred_element_type=F32)


def places(side, tok):
    n, half = side * side, tok // 2
    me = lax.axis_index("tp")
    core = me % 2
    chip = me // 2
    cy, cx = chip // side, chip % side
    diag = (cx + cy) % side
    pos_own = side * (cy * (1 - core) + cx * core) + diag
    pos_par = side * (cx * (1 - core) + cy * core) + diag

    def index_of(e, q):
        a, b = q // side, q % side
        o = (b - a + side) % side
        yy = a * (1 - e) + o * e
        xx = o * (1 - e) + a * e
        return (yy * side + xx) * 2 + e

    def token_row(s, rel, d):
        e = core if rel == 0 else 1 - core
        base = pos_own if rel == 0 else pos_par
        q = (base + n - s) % n if d == 0 else (base + s) % n
        return pl.multiple_of(index_of(e, q) * tok + half * d, half)

    return me, core, pos_own, token_row, index_of


def kernel(side, x_in_hbm, gy_in_hbm, ug_hbm, uu_hbm, wg_hbm, wu_hbm, wd_hbm, xin_hbm, gamma_hbm, gr_hbm, o_hbm, wo_hbm,
           ds_out, do_v, acc_g, acc_u, acc_d, acc_o, yb, ov, wo,
           xb, ugt, uut, ug, uu, wg, wu, wd, xin, gamma, gr,
           g_s, du_g, du_u, z_s, own_part, pp_send, pp_recv, rs_send, rs_recv, acc0,
           do_acc, o_pair,
           y_rs, y_rr, y_ps, y_pr, x_rs, x_rr, x_ps, x_pr,
           s_rs, s_rr, s_ps, s_pr, r_s, r_r, q_s, q_r, loc):
    n = side * side
    tok, hid = x_in_hbm.shape
    half = tok // 2
    ct = hid // TILES

    me, core, pos_own, token_row, index_of = places(side, tok)
    partner = me + 1 - 2 * core
    nxt = (index_of(core, (pos_own + 1) % n), index_of(core, (pos_own + n - 1) % n))

    def remote(src, dst, ssem, rsem, dev):
        return pltpu.make_async_remote_copy(src_ref=src, dst_ref=dst, send_sem=ssem, recv_sem=rsem,
                                            device_id={"tp": dev}, device_id_type=pl.DeviceIdType.MESH)

    def local(i):
        pairs = ((gy_in_hbm, yb.at[0, pl.ds(0, tok), :]), (x_in_hbm, xb.at[0, pl.ds(0, tok), :]),
                 (wd_hbm, wd), (ug_hbm, ugt), (uu_hbm, uut), (wg_hbm, wg), (wu_hbm, wu),
                 (xin_hbm, xin), (gamma_hbm, gamma), (gr_hbm, gr), (o_hbm, ov), (wo_hbm, wo))
        return pltpu.make_async_copy(pairs[i][0], pairs[i][1], loc.at[i])

    for i in range(12):
        local(i).start()

    barrier = pltpu.get_barrier_semaphore()
    for dev in (nxt[0], nxt[1], partner):
        pl.semaphore_signal(barrier, inc=1, device_id={"tp": dev}, device_id_type=pl.DeviceIdType.MESH)
    pl.semaphore_wait(barrier, 3)

    def rows_at(s, rel, d):
        return pl.ds(pl.multiple_of((s % 2) * (2 * tok) + rel * tok + d * half, half), half)

    def cols_of(c, pieces):
        return pl.ds(c * (hid // pieces), hid // pieces)

    def ring_copy(b, sems, s, d, c, pieces):
        cols = cols_of(c, pieces)
        m = sems[0].shape[2]
        return remote(b.at[(s // 2) % 3, rows_at(s, 0, d), cols], b.at[((s + 1) // 2) % 3, rows_at(s + 1, 0, d), cols],
                      sems[0].at[d, c, s % m], sems[1].at[d, c, (s + 1) % m], nxt[d])

    def pair_copy(b, sems, s, d, c, pieces):
        cols = cols_of(c, pieces)
        m = sems[0].shape[2]
        return remote(b.at[(s // 2) % 3, rows_at(s, 0, d), cols], b.at[(s // 2) % 3, rows_at(s, 1, d), cols],
                      sems[2].at[d, c, s % m], sems[3].at[d, c, s % m], partner)

    def between(s, lo, hi):
        return jnp.logical_and(s >= lo, s <= hi)

    def each(pieces, f, part=None):
        for c in part or range(pieces):
            for d in range(2):
                f(d, c, pieces)

    def forward(b, sems, s, pieces, part=None):

        def one(d, c, pieces):
            @pl.when(between(s, 1, n - 1))
            def _():
                ring_copy(b, sems, s - 1, d, c, pieces).wait_recv()

            @pl.when(between(s, 0, n - 2))
            def _():
                ring_copy(b, sems, s, d, c, pieces).start()

            @pl.when(between(s, 0, n - 1))
            def _():
                pair_copy(b, sems, s, d, c, pieces).start()
        each(pieces, one, part)

        @pl.when(between(s, 2, n + 1))
        def _():
            each(pieces, lambda d, c, p: pair_copy(b, sems, s - 2, d, c, p).wait_send(), part)

        @pl.when(between(s, 2, n))
        def _():
            each(pieces, lambda d, c, p: ring_copy(b, sems, s - 2, d, c, p).wait_send(), part)

    def pair_wait(b, sems, s, pieces, part=None):
        each(pieces, lambda d, c, p: pair_copy(b, sems, s, d, c, p).wait_recv(), part)

    y_sems, x_sems, s_sems = (y_rs, y_rr, y_ps, y_pr), (x_rs, x_rr, x_ps, x_pr), (s_rs, s_rr, s_ps, s_pr)

    early, late = tuple(range(X_PIECES // 2)), tuple(range(X_PIECES // 2, X_PIECES))

    def part_a(t):
        @pl.when(t == 0)
        def _():
            local(0).wait()
        forward(yb, y_sems, t, PIECES)

    def part_b(t):
        @pl.when(t == 0)
        def _():
            local(1).wait()
        forward(xb, x_sems, t, X_PIECES, early)

    def part_c(s):
        forward(xb, x_sems, s, X_PIECES, late)

    def task_1(k):
        @pl.when(k == 0)
        def _():
            for i in (2, 3, 4):
                local(i).wait()

            def turn(c, carry):
                cols = pl.ds(pl.multiple_of(c * 128, 128), 128)
                ug[cols, :] = ugt[:, cols].astype(F32).T.astype(BF16)
                uu[cols, :] = uut[:, cols].astype(F32).T.astype(BF16)
                return carry
            lax.fori_loop(0, ug.shape[0] // 128, turn, 0)
        pair_wait(yb, y_sems, 2 * k, PIECES)
        pair_wait(yb, y_sems, 2 * k + 1, PIECES)

    def task_1b(k):
        g_s[...] = dot(wd[...], yb[k % 3], NT).T
        for i in range(2):
            for rel in range(2):
                for d in range(2):
                    r0 = i * 2 * tok + rel * tok + d * half
                    row = token_row(2 * k + i, rel, d)
                    gate = ug[pl.ds(row, half), :].astype(F32)
                    up = uu[pl.ds(row, half), :].astype(F32)
                    sig = jax.nn.sigmoid(gate)
                    act = gate * sig
                    grad = g_s[pl.ds(r0, half), :]
                    z_s[pl.ds(r0, half), :] = (act * up).astype(BF16)
                    du_u[k, pl.ds(r0, half), :] = (grad * act).astype(BF16)
                    du_g[k, pl.ds(r0, half), :] = (grad * up * (sig * (1.0 + gate * (1.0 - sig)))).astype(BF16)

    def pp_copy(k):
        return remote(pp_send.at[k % 2], pp_recv.at[k % 2], q_s.at[k % 2], q_r.at[k % 2], partner)

    def task_2(k, lo, hi):
        ks = k % 2
        if lo == 0:
            @pl.when(k == 0)
            def _():
                local(5).wait()
                local(6).wait()

            @pl.when(k >= 2)
            def _():
                pp_copy(k - 2).wait_send()

        def body(c):
            cols = pl.ds(c * ct, ct)
            r = (dot(du_g[k], wg[:, cols], NN) + dot(du_u[k], wu[:, cols], NN)).astype(BF16)
            for i in range(2):
                own_part[ks, pl.ds(i * tok, tok), cols] = r[i * 2 * tok:i * 2 * tok + tok]
                pp_send[ks, pl.ds(i * tok, tok), cols] = r[i * 2 * tok + tok:(i + 1) * 2 * tok]
        for c in range(lo, hi):
            body(c)
        if hi == TILES:
            pp_copy(k).start()

    def task_3(k):
        def body(c):
            cols = pl.ds(c * ct, ct)
            acc_d[:, cols] += dot(z_s[...], yb[k % 3, :, cols], TN)
        for c in range(TILES):
            body(c)

    def task_4(k, lo, hi):
        if lo in (0, TILES // 2):
            part = early if lo == 0 else late
            pair_wait(xb, x_sems, 2 * k, X_PIECES, part)
            pair_wait(xb, x_sems, 2 * k + 1, X_PIECES, part)

        def body(c):
            cols = pl.ds(c * ct, ct)
            xt = xb[k % 3, :, cols]
            acc_g[:, cols] += dot(du_g[k], xt, TN)
            acc_u[:, cols] += dot(du_u[k], xt, TN)
        for c in range(lo, hi):
            body(c)

    def rs_copy(j, d, c, pieces):
        rows, cols = pl.ds(d * half, half), cols_of(c, pieces)
        return remote(rs_send.at[j % 2, rows, cols], rs_recv.at[(j + 1) % 3, rows, cols],
                      r_s.at[d, c, j % 2], r_r.at[d, c, (j + 1) % 3], nxt[d])

    def part_d(t, i):
        j = t - LAG_R
        ks = (j // 2) % 2
        rows = pl.ds(i * tok, tok)
        if i == 0:
            @pl.when(between(j, 0, n - 2))
            def _():
                pp_copy(j // 2).wait_recv()

            @pl.when(j == 0)
            def _():
                acc0[...] = own_part[ks, rows, :].astype(F32) + pp_recv[ks, rows, :].astype(F32)

        @pl.when(between(j, 3, n + 1))
        def _():
            each(PIECES, lambda d, c, p: rs_copy(j - 2, d, c, p).wait_send())

        def one(d, c, pieces):
            dr = pl.ds(d * half, half)
            pr = pl.ds(i * tok + d * half, half)
            cols = cols_of(c, pieces)

            @pl.when(between(j, 2, n))
            def _():
                rs_copy(j - 1, d, c, pieces).wait_recv()

            @pl.when(j == 1)
            def _():
                rs_send[j % 2, dr, cols] = (own_part[ks, pr, cols].astype(F32)
                                            + pp_recv[ks, pr, cols].astype(F32)).astype(BF16)

            @pl.when(between(j, 2, n - 1))
            def _():
                rs_send[j % 2, dr, cols] = (own_part[ks, pr, cols].astype(F32) + pp_recv[ks, pr, cols].astype(F32)
                                            + rs_recv[j % 3, dr, cols].astype(F32)).astype(BF16)

            @pl.when(between(j, 1, n - 1))
            def _():
                rs_copy(j, d, c, pieces).start()
        each(PIECES, one)

    def pair_body(kk, carry):
        t = 2 * kk
        part_a(t)

        @pl.when(kk == 0)
        def _():
            part_b(t)
            acc_d[...] = jnp.zeros_like(acc_d)
            acc_g[...] = jnp.zeros_like(acc_g)
            acc_u[...] = jnp.zeros_like(acc_u)
            acc_o[...] = jnp.zeros_like(acc_o)

        @pl.when(kk >= 1)
        def _():
            task_2(kk - 1, 0, TILES // 2)
            part_d(t, 1)
            task_2(kk - 1, TILES // 2, TILES)
            part_b(t)
            task_4(kk - 1, 0, TILES // 2)

        @pl.when(kk == n // 2)
        def _():
            part_c(t - n)
        t = 2 * kk + 1
        part_a(t)

        @pl.when(kk >= 1)
        def _():
            task_3(kk - 1)
            part_d(t, 0)

        @pl.when(kk < n // 2)
        def _():
            task_1(kk)
        part_b(t)

        @pl.when(kk < n // 2)
        def _():
            task_1b(kk)

        @pl.when(kk == n // 2)
        def _():
            part_c(t - n)
        return carry

    lax.fori_loop(0, n // 2 + 1, pair_body, 0)
    part_d(jnp.int32(n + 2), 1)
    part_c(jnp.int32(2))
    part_d(jnp.int32(n + 3), 0)

    for i in (7, 8, 9, 10, 11):
        local(i).wait()

    def norm(c, carry):
        rows = pl.ds(pl.multiple_of(c * 16, 16), 16)
        xf = xin[rows, :].astype(F32)
        inv = lax.rsqrt(jnp.mean(xf * xf, axis=-1, keepdims=True) + NORM_EPS)
        gx = (acc0[rows, :] + rs_recv[n % 3, rows, :].astype(F32)).astype(BF16)
        scaled = gx.astype(F32) * gamma[...].astype(F32).reshape(1, hid)
        proj = jnp.mean(scaled * xf, axis=-1, keepdims=True)
        ds = (gr[rows, :].astype(F32) + inv * (scaled - xf * (inv * inv) * proj)).astype(BF16)
        yb[0, rows, :] = ds
        ds_out[rows, :] = ds
        return carry
    lax.fori_loop(0, tok // 16, norm, 0)

    def o_task(m, c):
        cols = pl.ds(pl.multiple_of(c * ct, ct), ct)
        blk = yb[m % 3, :, cols]
        acc_o[:, cols] += dot(o_pair[...], blk, TN)
        part = dot(blk, wo[:, cols], NT)

        @pl.when(c == 0)
        def _():
            do_acc[...] = part

        @pl.when(c > 0)
        def _():
            do_acc[...] += part

    def o_rows(m):
        for i in range(2):
            for rel in range(2):
                for d in range(2):
                    yield i * 2 * tok + rel * tok + d * half, token_row(2 * m + i, rel, d)

    def o_begin(m):
        for r0, row in o_rows(m):
            o_pair[pl.ds(r0, half), :] = ov[pl.ds(row, half), :]

    def o_end(m):
        for r0, row in o_rows(m):
            do_v[pl.ds(row, half), :] = do_acc[pl.ds(r0, half), :].astype(BF16)

    def s_step(u, carry):
        m = u // 2 - 1

        @pl.when(jnp.logical_and(between(u, 2, n), u % 2 == 0))
        def _():
            each(SUBS, lambda d, c, p: pair_copy(yb, s_sems, 2 * m, d, c, p).wait_recv())
            each(SUBS, lambda d, c, p: pair_copy(yb, s_sems, 2 * m + 1, d, c, p).wait_recv())

        @pl.when(jnp.logical_and(between(u, 2, n - 1), u % 2 == 0))
        def _():
            o_begin(m)
        for c in range(SUBS):
            for d in range(2):
                @pl.when(between(u, 1, n - 1))
                def _():
                    ring_copy(yb, s_sems, u - 1, d, c, SUBS).wait_recv()

                @pl.when(u <= n - 2)
                def _():
                    ring_copy(yb, s_sems, u, d, c, SUBS).start()

                @pl.when(u <= n - 1)
                def _():
                    pair_copy(yb, s_sems, u, d, c, SUBS).start()

                @pl.when(between(u, 2, n + 1))
                def _():
                    pair_copy(yb, s_sems, u - 2, d, c, SUBS).wait_send()

                @pl.when(between(u, 2, n))
                def _():
                    ring_copy(yb, s_sems, u - 2, d, c, SUBS).wait_send()

            if c % 2 == 1:
                forward(xb, x_sems, u + 3, X_PIECES, (late[c // 2],))

            if c % (2 * SUBS // TILES) == 0:
                @pl.when(between(u, 2, n - 1))
                def _():
                    o_task(m, (u % 2) * (TILES // 2) + c * TILES // (2 * SUBS))

        @pl.when(jnp.logical_and(between(u, 2, n - 1), u % 2 == 1))
        def _():
            o_end(m)

        @pl.when(u == 0)
        def _():
            task_4(0, TILES // 2, TILES)

        @pl.when(jnp.logical_and(u <= n - 2, u % 2 == 1))
        def _():
            task_4((u + 1) // 2, TILES // 2, TILES)

        return carry

    lax.fori_loop(0, n + 2, s_step, 0)
    each(PIECES, lambda d, c, p: rs_copy(n - 1, d, c, p).wait_send())
    pp_copy(n // 2 - 2).wait_send()
    pp_copy(n // 2 - 1).wait_send()


def mega(side, *args):
    tok, hid = args[0].shape
    fl, rows = args[2].shape
    ol = args[10].shape[1]
    dma = pltpu.SemaphoreType.DMA
    ring = [dma((2, PIECES, SLOTS)) for _ in range(4)] + [dma((2, X_PIECES, SLOTS)) for _ in range(4)] + [dma((2, SUBS, 4)) for _ in range(4)]
    sems = ring + [dma((2, PIECES, 2)), dma((2, PIECES, 3)), dma((2,)), dma((2,)), dma((12,))]
    out_shape = (pltpu.VMEM((tok, hid), BF16), pltpu.VMEM((rows, ol), BF16), pltpu.VMEM((fl, hid), F32),
                 pltpu.VMEM((fl, hid), F32), pltpu.VMEM((fl, hid), F32), pltpu.VMEM((ol, hid), F32),
                 pltpu.VMEM((3, 4 * tok, hid), BF16), pltpu.VMEM((rows, ol), BF16), pltpu.VMEM((ol, hid), BF16))
    v = pltpu.VMEM
    blk = 4 * tok
    scratch = [
        v((3, blk, hid), BF16), v((fl, rows), BF16), v((fl, rows), BF16), v((rows, fl), BF16), v((rows, fl), BF16),
        v((fl, hid), BF16), v((fl, hid), BF16), v((fl, hid), BF16), v((tok, hid), BF16), v((hid,), BF16),
        v((tok, hid), BF16),
        v((blk, fl), F32), v((rows // blk, blk, fl), BF16), v((rows // blk, blk, fl), BF16), v((blk, fl), BF16),
        v((2, 2 * tok, hid), BF16), v((2, 2 * tok, hid), BF16), v((2, 2 * tok, hid), BF16),
        v((2, tok, hid), BF16), v((3, tok, hid), BF16), v((tok, hid), F32),
        v((blk, ol), F32), v((blk, ol), BF16)]
    anyspec = pl.BlockSpec(memory_space=pl.ANY)
    return pl.pallas_call(
        functools.partial(kernel, side),
        out_shape=out_shape,
        in_specs=[anyspec] * 12,
        out_specs=tuple([pl.BlockSpec(memory_space=pltpu.VMEM)] * 9),
        scratch_shapes=scratch + sems,
        compiler_params=pltpu.CompilerParams(collective_id=0, has_side_effects=True, vmem_limit_bytes=MEGA_VMEM),
    )(*args)


def flush_kernel(side, ds, do_v, acc_g, acc_u, acc_d, acc_o, yb, ov, wo,
                 ds_hbm, do_hbm, dwg_hbm, dwu_hbm, dwd_hbm, dwo_hbm, do_last, o_pair, sums, sem, row_sem, col_sem):
    n = side * side
    tok, hid = ds.shape
    half, ct, m = tok // 2, hid // TILES, n // 2 - 1
    token_row = places(side, tok)[3]
    pairs = ((do_v, do_hbm), (ds, ds_hbm), (acc_g, dwg_hbm), (acc_u, dwu_hbm), (acc_d, dwd_hbm))
    copies = [pltpu.make_async_copy(a, b, sem.at[i]) for i, (a, b) in enumerate(pairs)]
    for c in copies:
        c.start()
    spots = [(i * 2 * tok + rel * tok + d * half, token_row(2 * m + i, rel, d))
             for i in range(2) for rel in range(2) for d in range(2)]
    for r0, row in spots:
        o_pair[pl.ds(r0, half), :] = ov[pl.ds(row, half), :]
    col_copies = []
    for c in range(TILES):
        cols = pl.ds(c * ct, ct)
        sums[:, cols] = acc_o[:, cols] + dot(o_pair[...], yb[m % 3, :, cols], TN)
        col_copies.append(pltpu.make_async_copy(sums.at[:, cols], dwo_hbm.at[:, cols], col_sem.at[c]))
        col_copies[-1].start()
    do_last[...] = dot(yb[m % 3], wo[...], NT).astype(BF16)
    copies[0].wait()
    row_copies = [pltpu.make_async_copy(do_last.at[pl.ds(r0, half), :], do_hbm.at[pl.ds(row, half), :], row_sem.at[i])
                  for i, (r0, row) in enumerate(spots)]
    for c in row_copies:
        c.start()
    for c in copies[1:] + col_copies + row_copies:
        c.wait()


def flush(side, *arrays):
    outs = arrays[:6]
    tok, hid = outs[0].shape
    ol = outs[5].shape[0]
    dma = pltpu.SemaphoreType.DMA
    return pl.pallas_call(
        functools.partial(flush_kernel, side),
        out_shape=tuple(pltpu.HBM(a.shape, a.dtype) for a in outs),
        in_specs=[pl.BlockSpec(memory_space=pltpu.VMEM)] * len(arrays),
        out_specs=tuple([pl.BlockSpec(memory_space=pltpu.HBM)] * len(outs)),
        scratch_shapes=[pltpu.VMEM((4 * tok, ol), BF16), pltpu.VMEM((4 * tok, ol), BF16), pltpu.VMEM((ol, hid), F32),
                        dma((5,)), dma((8,)), dma((TILES,))],
        compiler_params=pltpu.CompilerParams(vmem_limit_bytes=FLUSH_VMEM),
    )(*[pltpu.with_memory_space_constraint(a, pltpu.VMEM) for a in arrays])


def solution(mesh):
    token_spec = P(("dp", "tp"), None)
    split_cols = P("dp", "tp")
    weight_cols = P(None, "tp")
    weight_rows = P("tp", None)
    side = math.isqrt(mesh.shape["tp"] // 2)

    def local_backward(x_norm, grad_y, u_gate, u_up, w_gate, w_up, w_down, x_in, gamma, grad_res, attn_out, w_out):
        grad_sum, grad_attn, gw_gate, gw_up, gw_down, gw_out = flush(side, *mega(
            side, x_norm, grad_y, u_gate.T, u_up.T, w_gate.T, w_up.T, w_down, x_in, gamma,
            grad_res, attn_out, w_out))
        return grad_sum, grad_attn, gw_gate.T, gw_up.T, gw_down, gw_out

    return jax.shard_map(
        local_backward,
        mesh=mesh,
        in_specs=(token_spec, token_spec, split_cols, split_cols, weight_cols, weight_cols, weight_rows,
                  token_spec, P(None), token_spec, split_cols, weight_rows),
        out_specs=(token_spec, split_cols, split_cols, split_cols, token_spec, token_spec),
        check_vma=False,
    )
```
